256 devices in a mesh: section: 8 (over x, core), wide: 32 (over z, y).
Axes of the slice: x: 4, y: 4, z: 8, core: 2. Of those that a mesh axis runs over, the one named last changes fastest.
Arguments:
- stream: bfloat16 [8, 2048, 2048], P('section', 'wide'), may hold values from -3 to 3
- mixer_gain: float32 [8, 2048], P('section'), may hold values from 0.1 to 1.9
- ssm_weight: bfloat16 [8, 2048, 160], P('section'), may hold values from -0.125 to 0.125
- decay_rate: float32 [8, 32], P('section'), may hold values from 2.4414063e-05 to 0.04
- skip_gain: float32 [8, 32], P('section'), may hold values from 0.5 to 1.5
- mixed_gain: float32 [8, 2048], P('section'), may hold values from 0.1 to 1.9
- ffn_gain: float32 [8, 2048], P('section'), may hold values from 0.1 to 1.9
- router_weight: bfloat16 [8, 2048, 4], P('section'), may hold values from -0.125 to 0.125
- expert_ids: int32 [8, 2048, 2], P('section', 'wide'), may hold values from 0 to 3, all different within a row; in each aligned block of 64 rows (0 to 63, 64 to 127, ..., all dimensions but the last counted through in order) at most 40 rows name the same one
- gate_weight: bfloat16 [8, 2048, 28672], P('section', None, 'wide'), may hold values from -0.125 to 0.125
- up_weight: bfloat16 [8, 2048, 28672], P('section', None, 'wide'), may hold values from -0.125 to 0.125
- down_weight: bfloat16 [8, 28672, 2048], P('section', 'wide'), may hold values from -0.0625 to 0.0625
Outputs:
- carried: bfloat16 [8, 2048, 2048], P('section', 'wide')
The draws below stay inside these ranges and needn't reach their ends.
Inputs may be any that keep to these rules, and one draw needn't show every extreme that they name: `expert_ids`: A token's 2 experts differ. Among the tokens of one device, no expert is named by more than 40 of them, a bound that some block reaches.
All inputs are finite; a program needn't handle non-finite values.
Results may differ from the reference program's by a relative error of at most 0.0085.
Values may be sent and summed in bfloat16 or wider, within the bound.
No kernel may reach another device: no remote copies, remote signals or barrier semaphores. Data moves between devices by JAX's collectives and lax.ppermute only.
A program may use at most 128 MiB of HBM per device.

```python
import math
import jax
import jax.numpy as jnp
import numpy as np
from jax import lax

D = 2048
HEADS = 32
HEAD_DIM = 64
STATE = 64
EXPERTS = 4
FF = 7168
TOP = 2
TOK_DEV = 64
CAP = 40
TOKENS = 2048
SECTIONS = 8
N_WIDE = 32


def level_of(stream_key, dims, split, low, largest):
    factor_of, own = 1.0, jax.random.fold_in(stream_key, 6)
    for axis_at, shards_of in split:
        draws = jnp.exp(jax.random.uniform(jax.random.fold_in(own, axis_at), (shards_of,), jnp.float32, low / len(split), largest / len(split)))
        factor_of = factor_of * jnp.repeat(draws, dims[axis_at] // shards_of).reshape([-1 if axis == axis_at else 1 for axis in range(len(dims))])
    return factor_of


def shared_out(rng, own, number, rows, count, top, limit, lean):
    sequence = jax.random.permutation(rng, count)
    heavy_load, common = portions_of(count, rows * top, limit, lean, True), portions_of(count, rows * top, limit, lean, False)
    places = jnp.arange(count)

    def named(tallies, rotation):
        used = int((tallies > 0).sum())
        fixed = max(1, used // 4)
        passed = fixed + (places - fixed + rotation * (used - fixed)) % max(1, count - fixed)
        return jnp.zeros((count,), jnp.int32).at[sequence[jnp.where(places < fixed, places, passed)]].set(jnp.asarray(tallies, jnp.int32))

    tallies = jnp.where(number % 4 == 0, named(heavy_load, number // 4), named(common, number - number // 4 - 1))
    mixed = jax.random.permutation(jax.random.fold_in(own, 3), count)
    source_of, sink = mixed[0:count // 2 * 2:2], mixed[1:count // 2 * 2:2]
    slack = jnp.minimum(tallies[source_of] - 1, limit - tallies[sink]) // 2
    slack = jnp.where((source_of == sequence[0]) | (sink == sequence[0]) | (tallies[sink] == 0), 0, jnp.maximum(slack, 0))
    passed = jax.random.randint(jax.random.fold_in(own, 4), (count // 2,), 0, 1 << 20) % (slack + 1)
    tallies = tallies.at[source_of].add(-passed).at[sink].add(passed)
    labels = jnp.searchsorted(jnp.cumsum(tallies), jnp.arange(rows * top), side="right").astype(jnp.int32)
    table = labels.reshape(top, rows).T
    table = table[jax.random.permutation(jax.random.fold_in(own, 1), rows)]
    rotation = jax.random.randint(jax.random.fold_in(own, 2), (rows, 1), 0, top)
    return jnp.take_along_axis(table, (jnp.arange(top)[None, :] + rotation) % top, axis=1)


def portions_of(amount, total, bound, skew, full):
    loads = [(1 << 20) // math.isqrt(grade ** skew) + 1 for grade in range(1, amount + 1)]
    largest = bound if full else min(bound, max(-(-total // amount), total * loads[0] // sum(loads)))
    least = 1 if total - largest >= amount - 1 else 0
    counts, rest = [largest] + [least] * (amount - 1), total - largest - least * (amount - 1)
    while rest > 0:
        movable = [i for i in range(1, amount) if counts[i] < largest] or [i for i in range(1, amount) if counts[i] < bound]
        whole, remaining = sum([loads[i] for i in movable]), rest
        for i in movable:
            extra = min(bound - counts[i], max(1, remaining * loads[i] // whole), rest)
            counts[i] = counts[i] + extra
            rest = rest - extra
    return np.array(counts)


def bell_draw(rng, extent, spread, most, split=(), held_as=jnp.bfloat16):
    result = spread * jax.random.normal(rng, extent, jnp.float32)
    if split:
        result = result * level_of(rng, extent, split, -0.22, 0.18)
    return jnp.clip(result, -most, most).astype(held_as)


def setup_inputs(seed: int = 0) -> dict:
    seeds = jax.random.split(jax.random.key(seed), 13)
    stream = bell_draw(seeds[0], (SECTIONS, TOKENS, D), 0.5, 3.0, ((0, 8), (1, 32)))
    mixer_gain = jnp.clip(1.0 + 0.18 * jax.random.normal(seeds[1], (SECTIONS, D), jnp.float32), 0.1, 1.9)
    ssm_weight = bell_draw(seeds[2], (SECTIONS, D, 2 * STATE + HEADS), D ** -0.5, 0.125, ((0, 8),))
    decay_rate = jnp.clip(jnp.exp(math.log(0.04) - 7.4014754 * jax.random.uniform(seeds[3], (SECTIONS, HEADS), jnp.float32) ** level_of(seeds[3], (SECTIONS, HEADS), ((0, 8),), -0.2, 0.2)), 2.441406286379788e-05, 0.04)
    skip_gain = jnp.clip(0.5 + 1.0 * jax.random.uniform(seeds[4], (SECTIONS, HEADS), jnp.float32) ** level_of(seeds[4], (SECTIONS, HEADS), ((0, 8),), -0.2, 0.2), 0.5, 1.5)
    mixed_gain = jnp.clip(1.0 + 0.18 * jax.random.normal(seeds[5], (SECTIONS, D), jnp.float32), 0.1, 1.9)
    ffn_gain = jnp.clip(1.0 + 0.18 * jax.random.normal(seeds[6], (SECTIONS, D), jnp.float32), 0.1, 1.9)
    router_weight = bell_draw(seeds[7], (SECTIONS, D, EXPERTS), D ** -0.5, 0.125, ((0, 8),))
    expert_ids_keys = jax.random.split(jax.random.fold_in(seeds[8], 1), SECTIONS * TOKENS // TOK_DEV)
    expert_ids_turns = jax.random.permutation(jax.random.fold_in(seeds[8], 3), SECTIONS * TOKENS // TOK_DEV)
    expert_ids = jax.vmap(lambda own, number: shared_out(jax.random.fold_in(seeds[8], 2), own, number, TOK_DEV, EXPERTS, TOP, CAP, 2))(expert_ids_keys, expert_ids_turns).reshape((SECTIONS, TOKENS, TOP))
    gate_weight = bell_draw(seeds[9], (SECTIONS, D, EXPERTS * FF), D ** -0.5, 0.125, ((0, 8), (2, 32)))
    up_weight = bell_draw(seeds[10], (SECTIONS, D, EXPERTS * FF), D ** -0.5, 0.125, ((0, 8), (2, 32)))
    down_weight = bell_draw(seeds[11], (SECTIONS, EXPERTS * FF, D), FF ** -0.5, 0.0625, ((0, 8), (1, 32)))
    return dict(stream=stream, mixer_gain=mixer_gain, ssm_weight=ssm_weight, decay_rate=decay_rate, skip_gain=skip_gain, mixed_gain=mixed_gain, ffn_gain=ffn_gain, router_weight=router_weight, expert_ids=expert_ids, gate_weight=gate_weight, up_weight=up_weight, down_weight=down_weight)


EPSILON = 1e-05
HIGHEST_PREC = lax.Precision.HIGHEST

def rms_scale(values, gain_row):
    mean_sq = lax.optimization_barrier(jnp.mean(values * values, axis=-1, keepdims=True))
    return values * lax.rsqrt(mean_sq + EPSILON) * gain_row

def route_slots(id_rows):
    flat_ids = id_rows.reshape(-1).astype(jnp.int32)
    one_hot = (flat_ids[:, None] == jnp.arange(EXPERTS, dtype=jnp.int32)[None, :]).astype(jnp.int32)
    running = jnp.cumsum(one_hot, axis=0) - 1
    slot_ids = lax.optimization_barrier(jnp.sum(one_hot * running, axis=1)).astype(jnp.int32)
    return flat_ids * CAP + slot_ids

def mixer_block(inputs, mixer_gain, ssm_weight, decay_rate, skip_gain, mixed_gain):
    residual = inputs.astype(jnp.float32)
    normed = rms_scale(residual, mixer_gain).astype(jnp.bfloat16)
    projected = jnp.dot(normed, ssm_weight, preferred_element_type=jnp.float32)
    b_rows = projected[:, :STATE] / float(STATE)
    c_rows = projected[:, STATE:2 * STATE] / math.sqrt(STATE)
    step_size = jax.nn.softplus(projected[:, 2 * STATE:])
    values = normed.astype(jnp.float32)
    decay_cols = jnp.repeat(jnp.exp(-step_size * decay_rate[None, :]), HEAD_DIM, axis=1)
    step_cols = jnp.repeat(step_size, HEAD_DIM, axis=1)

    def advance(carry_state, inputs_row):
        decay_row, step_row, b_row, c_row, value_row = inputs_row
        carry_state = decay_row[None, :] * carry_state + b_row[:, None] * (step_row * value_row)[None, :]
        return (carry_state, jnp.dot(c_row, carry_state, precision=HIGHEST_PREC))
    start_state = jnp.zeros((STATE, D), jnp.float32)
    _, readout = lax.scan(advance, start_state, (decay_cols, step_cols, b_rows, c_rows, values))
    mixed = readout + values * jnp.repeat(skip_gain, HEAD_DIM)[None, :]
    return residual + rms_scale(mixed, mixed_gain)

def expert_layer(residual, ffn_gain, router_weight, id_rows, gate_weight, up_weight, down_weight):
    routed = rms_scale(residual, ffn_gain).astype(jnp.bfloat16)
    logits = jnp.dot(routed, router_weight, preferred_element_type=jnp.float32)
    chosen = jnp.take_along_axis(logits, id_rows, axis=1)
    first_share = jax.nn.sigmoid(chosen[:, 0] - chosen[:, 1])
    shares = jnp.stack([first_share, 1.0 - first_share], axis=1)
    blocks = id_rows.reshape(N_WIDE, TOK_DEV, TOP)
    targets = jax.vmap(route_slots)(blocks)
    experts_of = blocks.reshape(N_WIDE, TOK_DEV * TOP).astype(jnp.int32)
    offsets = (jnp.arange(N_WIDE, dtype=jnp.int32) * CAP)[:, None]
    rows_at = (targets - experts_of * CAP + offsets).reshape(-1)
    experts_flat = experts_of.reshape(-1)
    doubled = jnp.repeat(routed, TOP, axis=0)
    buffers = jnp.zeros((EXPERTS, N_WIDE * CAP, D), jnp.bfloat16).at[experts_flat, rows_at].set(doubled)
    members = N_WIDE // EXPERTS
    part_width = FF // members
    gate_all = gate_weight.reshape(D, EXPERTS, FF).transpose(1, 0, 2)
    up_all = up_weight.reshape(D, EXPERTS, FF).transpose(1, 0, 2)
    down_all = down_weight.reshape(EXPERTS, FF, D)

    def one_expert(pieces):
        rows_in, gate_one, up_one, down_one = pieces
        gate_pre = jnp.dot(rows_in, gate_one, preferred_element_type=jnp.float32)
        up_pre = jnp.dot(rows_in, up_one, preferred_element_type=jnp.float32)
        hidden = (jax.nn.silu(gate_pre) * up_pre).astype(jnp.bfloat16)
        split_hidden = hidden.reshape(-1, members, part_width).astype(jnp.float32)
        split_down = down_one.reshape(members, part_width, D).astype(jnp.float32)
        partials = jnp.einsum('rgf,gfd->grd', split_hidden, split_down, precision=HIGHEST_PREC)
        return lax.optimization_barrier(jnp.sum(partials.astype(jnp.bfloat16).astype(jnp.float32), axis=0))
    answers = lax.map(one_expert, (buffers, gate_all, up_all, down_all))
    picked = answers[experts_flat, rows_at].reshape(TOKENS, TOP, D)
    return (residual + lax.optimization_barrier(jnp.sum(picked * shares[:, :, None], axis=1))).astype(jnp.bfloat16)

def reference(stream, mixer_gain, ssm_weight, decay_rate, skip_gain, mixed_gain, ffn_gain, router_weight, expert_ids, gate_weight, up_weight, down_weight):
    outputs = []
    for section_index in range(SECTIONS):
        residual = mixer_block(stream[section_index], mixer_gain[section_index], ssm_weight[section_index], decay_rate[section_index], skip_gain[section_index], mixed_gain[section_index])
        outputs.append(expert_layer(residual, ffn_gain[section_index], router_weight[section_index], expert_ids[section_index], gate_weight[section_index], up_weight[section_index], down_weight[section_index]))
    return jnp.roll(jnp.stack(outputs), 1, axis=0)
```

```python
import math

import jax
import jax.numpy as jnp
from jax import lax
from jax.experimental import pallas as pl
from jax.experimental.pallas import tpu as pltpu
from jax.sharding import Mesh
from jax.sharding import PartitionSpec as P

HEADS = 32
HEAD_DIM = 64
STATE = 64
EXPERTS = 4
TOP = 2
CAP = 40
NZ = 8
NY = 4
WIDE = ("wide_0", "wide_1")
EPSILON = 1e-05
CHUNKS = ((0, 1, 7, 4), (2, 6, 3, 5))


def passed_along(value, axis, by):
    length = lax.axis_size(axis)
    return lax.ppermute(value, axis, [(i, (i + by) % length) for i in range(length)])


def rms_scale(values, gain_row):
    mean_sq = jnp.mean(values * values, axis=-1, keepdims=True)
    return values * lax.rsqrt(mean_sq + EPSILON) * gain_row


def split3(values):
    hi = lax.reduce_precision(values, 8, 7)
    rest = values - hi
    mid = lax.reduce_precision(rest, 8, 7)
    return hi, mid, rest - mid


def route_slots(id_rows):
    flat_ids = id_rows.reshape(-1)
    one_hot = (
        flat_ids[:, None] == lax.broadcasted_iota(jnp.int32, (flat_ids.shape[0], EXPERTS), 1)
    ).astype(jnp.int32)
    running = jnp.cumsum(one_hot, axis=0) - 1
    slot_ids = jnp.sum(one_hot * running, axis=1)
    return slot_ids


def prefix_kernel(arrived_ref, out_ref):
    def step(k, carry):
        out_ref[k] = carry.astype(jnp.bfloat16)
        block = arrived_ref[k].astype(jnp.float32)
        decay = block[32:33] + block[33:34] + block[34:35]
        return carry * decay + block[:32]

    lax.fori_loop(0, NZ * NY, step, jnp.zeros((32, 128), jnp.float32))


def prefix_states(arrived):
    return pl.pallas_call(
        prefix_kernel,
        out_shape=jax.ShapeDtypeStruct((NZ * NY, 32, 128), jnp.bfloat16),
        in_specs=[pl.BlockSpec(memory_space=pltpu.VMEM)],
        out_specs=pl.BlockSpec(memory_space=pltpu.VMEM),
        name="prefix_states",
    )(arrived)


def carried_states(local_state, decay_cols):
    pieces = (
        local_state.astype(jnp.bfloat16).reshape(2, 32, 16, 128).transpose(2, 0, 1, 3)
    ).reshape(32, 32, 128)
    decays = jnp.stack(split3(decay_cols), axis=0).astype(jnp.bfloat16)
    decays = jnp.repeat(decays.reshape(3, 16, 128).transpose(1, 0, 2), 2, axis=0)
    payload = jnp.concatenate([pieces, decays, jnp.zeros((32, 13, 128), jnp.bfloat16)], axis=1)
    arrived = lax.all_to_all(payload, WIDE, split_axis=0, concat_axis=0, tiled=True)
    back = lax.all_to_all(
        prefix_states(arrived), WIDE, split_axis=0, concat_axis=0, tiled=True
    )
    return back.reshape(16, 2, 32, 128).transpose(1, 2, 0, 3).reshape(STATE, -1)


def mixer_block(inputs, mixer_gain, ssm_weight, decay_rate, skip_gain, mixed_gain):
    residual = inputs.astype(jnp.float32)
    normed = rms_scale(residual, mixer_gain).astype(jnp.bfloat16)
    projected = jnp.dot(normed, ssm_weight, preferred_element_type=jnp.float32)
    b_rows = projected[:, :STATE] / float(STATE)
    c_rows = projected[:, STATE : 2 * STATE] / math.sqrt(STATE)
    step_size = jax.nn.softplus(projected[:, 2 * STATE :])
    cumulative = jnp.cumsum(-step_size * decay_rate[None, :], axis=0)
    seq_len = inputs.shape[0]
    values = normed.astype(jnp.float32)
    head_values = values.reshape(seq_len, HEADS, HEAD_DIM)
    tail_weights = jnp.exp(cumulative[-1][None, :] - cumulative) * step_size
    weighted = (tail_weights[:, :, None] * head_values).reshape(seq_len, -1)
    local_state = jnp.dot(b_rows.T, weighted)
    decay_cols = jnp.repeat(jnp.exp(cumulative[-1]), HEAD_DIM)
    carried_in = carried_states(local_state, decay_cols)
    later_mask = (
        lax.broadcasted_iota(jnp.int32, (seq_len, seq_len), 0)
        >= lax.broadcasted_iota(jnp.int32, (seq_len, seq_len), 1)
    )[:, :, None]
    log_gaps = cumulative[:, None, :] - cumulative[None, :, :]
    kernel = jnp.where(later_mask, jnp.exp(jnp.where(later_mask, log_gaps, 0.0)), 0.0)
    intersections = jnp.dot(c_rows, b_rows.T)
    mixing = intersections[:, :, None] * kernel * step_size[None, :, :]
    within = jnp.einsum("tsh,shp->thp", mixing, head_values).reshape(seq_len, -1)
    carried_part = jnp.dot(
        c_rows.astype(jnp.bfloat16), carried_in, preferred_element_type=jnp.float32
    ) * jnp.repeat(jnp.exp(cumulative), HEAD_DIM, axis=1)
    mixed = within + carried_part + values * jnp.repeat(skip_gain, HEAD_DIM)[None, :]
    return residual + rms_scale(mixed, mixed_gain)


def expert_rows(rows, gate_part, up_part, down_part):
    gate_pre = jnp.dot(rows, gate_part, preferred_element_type=jnp.float32)
    up_pre = jnp.dot(rows, up_part, preferred_element_type=jnp.float32)
    hidden = (jax.nn.silu(gate_pre) * up_pre).astype(jnp.bfloat16)
    return jnp.dot(hidden, down_part, preferred_element_type=jnp.float32).astype(jnp.bfloat16)


def added(one, other):
    return (one.astype(jnp.float32) + other.astype(jnp.float32)).astype(jnp.bfloat16)


def expert_layer(residual, ffn_gain, router_weight, id_rows, gate_part, up_part, down_part):
    tok_rows = residual.shape[0]
    features = residual.shape[1]
    zi = lax.axis_index("wide_0")
    slots = route_slots(id_rows).reshape(tok_rows, TOP)
    routed = rms_scale(residual, ffn_gain).astype(jnp.bfloat16)
    logits = jnp.dot(routed, router_weight, preferred_element_type=jnp.float32)
    chosen = jnp.take_along_axis(logits, id_rows, axis=1)
    first_share = jax.nn.sigmoid(chosen[:, 0] - chosen[:, 1])
    shares = jnp.stack([first_share, 1.0 - first_share], axis=1)

    col_expert = ((zi + lax.broadcasted_iota(jnp.int32, (NZ, CAP), 0)) % NZ // 2).reshape(-1)
    col_slot = lax.broadcasted_iota(jnp.int32, (NZ, CAP), 1).reshape(-1)
    hits = [
        (id_rows[:, k][:, None] == col_expert[None, :]) & (slots[:, k][:, None] == col_slot[None, :])
        for k in range(TOP)
    ]
    placing = (hits[0] | hits[1]).astype(jnp.bfloat16)
    combine = jnp.where(hits[0], shares[:, 0:1], 0.0) + jnp.where(hits[1], shares[:, 1:2], 0.0)
    packed = lax.dot_general(
        placing, routed, (((0,), (0,)), ((), ())), preferred_element_type=jnp.float32
    ).astype(jnp.bfloat16).reshape(NZ, CAP, features)

    arrived = {k: packed[0] if k == 0 else passed_along(packed[k], "wide_0", k) for chunk in CHUNKS for k in chunk}
    answers = {}
    for chunk in CHUNKS:
        own = jnp.concatenate([arrived[k] for k in chunk], axis=0)
        half = own.shape[0] // 2
        left = passed_along(own, "wide_1", 1)
        right = passed_along(own, "wide_1", -1)
        far_a = passed_along(left[:half], "wide_1", 1)
        far_b = passed_along(right[half:], "wide_1", -1)
        rows = jnp.concatenate([own, left, right, far_a, far_b], axis=0)
        out = expert_rows(rows, gate_part, up_part, down_part)
        full = own.shape[0]
        o_own, o_left, o_right = out[:full], out[full : 2 * full], out[2 * full : 3 * full]
        o_far_a, o_far_b = out[3 * full : 3 * full + half], out[3 * full + half :]
        mid_a = passed_along(o_far_a, "wide_1", -1)
        mid_b = passed_along(o_far_b, "wide_1", 1)
        to_left = jnp.concatenate([added(o_left[:half], mid_a), o_left[half:]], axis=0)
        to_right = jnp.concatenate([o_right[:half], added(o_right[half:], mid_b)], axis=0)
        from_left = passed_along(to_left, "wide_1", -1)
        from_right = passed_along(to_right, "wide_1", 1)
        summed = (
            o_own.astype(jnp.float32)
            + from_left.astype(jnp.float32)
            + from_right.astype(jnp.float32)
        ).astype(jnp.bfloat16)
        for i, k in enumerate(chunk):
            block = summed[i * CAP : (i + 1) * CAP]
            answers[k] = block if k == 0 else passed_along(block, "wide_0", -k)
    stacked = jnp.concatenate([answers[k] for k in range(NZ)], axis=0)
    combine_hi = lax.reduce_precision(combine, 8, 7)
    combine_lo = combine - combine_hi
    mixed_out = jnp.dot(
        combine_hi.astype(jnp.bfloat16), stacked, preferred_element_type=jnp.float32
    ) + jnp.dot(combine_lo.astype(jnp.bfloat16), stacked, preferred_element_type=jnp.float32)
    return (residual + mixed_out).astype(jnp.bfloat16)


def local(
    stream,
    mixer_gain,
    ssm_weight,
    decay_rate,
    skip_gain,
    mixed_gain,
    ffn_gain,
    router_weight,
    expert_ids,
    gate_weight,
    up_weight,
    down_weight,
):
    residual = mixer_block(
        stream[0], mixer_gain[0], ssm_weight[0], decay_rate[0], skip_gain[0], mixed_gain[0]
    )
    finished = expert_layer(
        residual,
        ffn_gain[0],
        router_weight[0],
        expert_ids[0],
        gate_weight[0],
        up_weight[0],
        down_weight[0],
    )
    return passed_along(finished[None], "section", 1)


def solution(mesh):
    finer = Mesh(
        mesh.devices.reshape(mesh.shape["section"], NZ, NY), ("section", "wide_0", "wide_1")
    )
    placed = (
        P("section", WIDE, None),
        P("section", None),
        P("section", None, None),
        P("section", None),
        P("section", None),
        P("section", None),
        P("section", None),
        P("section", None, None),
        P("section", WIDE, None),
        P("section", None, WIDE),
        P("section", None, WIDE),
        P("section", WIDE, None),
    )
    return jax.shard_map(
        local, mesh=finer, in_specs=placed, out_specs=P("section", WIDE, None), check_vma=False
    )
```

```python
import functools
import math

import jax
import jax.numpy as jnp
from jax import lax
from jax.experimental import pallas as pl
from jax.experimental.pallas import tpu as pltpu
from jax.sharding import Mesh
from jax.sharding import PartitionSpec as P

HEADS = 32
HEAD_DIM = 64
STATE = 64
EXPERTS = 4
TOP = 2
CAP = 40
NZ = 8
NY = 4
WIDE = ("wide_0", "wide_1")
EPSILON = 1e-05
CHUNKS = ((0, 1, 7, 4), (2, 6, 3, 5))


def passed_along(value, axis, by):
    length = lax.axis_size(axis)
    return lax.ppermute(value, axis, [(i, (i + by) % length) for i in range(length)])


def rms_scale(values, gain_row):
    mean_sq = jnp.mean(values * values, axis=-1, keepdims=True)
    return values * lax.rsqrt(mean_sq + EPSILON) * gain_row


def split3(values):
    hi = lax.reduce_precision(values, 8, 7)
    rest = values - hi
    mid = lax.reduce_precision(rest, 8, 7)
    return hi, mid, rest - mid


def route_slots(id_rows):
    flat_ids = id_rows.reshape(-1)
    one_hot = (
        flat_ids[:, None] == lax.broadcasted_iota(jnp.int32, (flat_ids.shape[0], EXPERTS), 1)
    ).astype(jnp.int32)
    running = jnp.cumsum(one_hot, axis=0) - 1
    slot_ids = jnp.sum(one_hot * running, axis=1)
    return slot_ids


def prefix_kernel(arrived_ref, out_ref):
    def step(k, carry):
        out_ref[k] = carry.astype(jnp.bfloat16)
        block = arrived_ref[k].astype(jnp.float32)
        decay = block[32:33] + block[33:34] + block[34:35]
        return carry * decay + block[:32]

    lax.fori_loop(0, NZ * NY, step, jnp.zeros((32, 128), jnp.float32))


def prefix_states(arrived):
    return pl.pallas_call(
        prefix_kernel,
        out_shape=jax.ShapeDtypeStruct((NZ * NY, 32, 128), jnp.bfloat16),
        in_specs=[pl.BlockSpec(memory_space=pltpu.VMEM)],
        out_specs=pl.BlockSpec(memory_space=pltpu.VMEM),
        name="prefix_states",
    )(arrived)


def carried_states(local_state, decay_cols):
    pieces = (
        local_state.astype(jnp.bfloat16).reshape(2, 32, 16, 128).transpose(2, 0, 1, 3)
    ).reshape(32, 32, 128)
    decays = jnp.stack(split3(decay_cols), axis=0).astype(jnp.bfloat16)
    decays = jnp.repeat(decays.reshape(3, 16, 128).transpose(1, 0, 2), 2, axis=0)
    payload = jnp.concatenate([pieces, decays, jnp.zeros((32, 5, 128), jnp.bfloat16)], axis=1)
    arrived = lax.all_to_all(payload, WIDE, split_axis=0, concat_axis=0, tiled=True)
    back = lax.all_to_all(
        prefix_states(arrived), WIDE, split_axis=0, concat_axis=0, tiled=True
    )
    return back.reshape(16, 2, 32, 128).transpose(1, 2, 0, 3).reshape(STATE, -1)


def mixer_block(inputs, mixer_gain, ssm_weight, decay_rate, skip_gain, mixed_gain):
    residual = inputs.astype(jnp.float32)
    normed = rms_scale(residual, mixer_gain).astype(jnp.bfloat16)
    projected = jnp.dot(normed, ssm_weight, preferred_element_type=jnp.float32)
    b_rows = projected[:, :STATE] / float(STATE)
    c_rows = projected[:, STATE : 2 * STATE] / math.sqrt(STATE)
    step_size = jax.nn.softplus(projected[:, 2 * STATE :])
    cumulative = jnp.cumsum(-step_size * decay_rate[None, :], axis=0)
    seq_len = inputs.shape[0]
    values = normed.astype(jnp.float32)
    head_values = values.reshape(seq_len, HEADS, HEAD_DIM)
    tail_weights = jnp.exp(cumulative[-1][None, :] - cumulative) * step_size
    weighted = (tail_weights[:, :, None] * head_values).reshape(seq_len, -1)
    local_state = jnp.dot(b_rows.T, weighted)
    decay_cols = jnp.repeat(jnp.exp(cumulative[-1]), HEAD_DIM)
    carried_in = carried_states(local_state, decay_cols)
    later_mask = (
        lax.broadcasted_iota(jnp.int32, (seq_len, seq_len), 0)
        >= lax.broadcasted_iota(jnp.int32, (seq_len, seq_len), 1)
    )[:, :, None]
    log_gaps = cumulative[:, None, :] - cumulative[None, :, :]
    kernel = jnp.where(later_mask, jnp.exp(jnp.where(later_mask, log_gaps, 0.0)), 0.0)
    intersections = jnp.dot(c_rows, b_rows.T)
    mixing = intersections[:, :, None] * kernel * step_size[None, :, :]
    within = jnp.einsum("tsh,shp->thp", mixing, head_values).reshape(seq_len, -1)
    carried_part = jnp.dot(
        c_rows.astype(jnp.bfloat16), carried_in, preferred_element_type=jnp.float32
    ) * jnp.repeat(jnp.exp(cumulative), HEAD_DIM, axis=1)
    mixed = within + carried_part + values * jnp.repeat(skip_gain, HEAD_DIM)[None, :]
    return residual + rms_scale(mixed, mixed_gain)


def expert_kernel(sizes, tile, out_tile, *refs):
    n = len(sizes)
    pieces, (gate, up, down), outs = refs[:n], refs[n : n + 3], refs[n + 3 : 2 * n + 3]
    rows, gate_up, downs, hidden, sem_in, sem_down = refs[2 * n + 3 :]
    tiles, out_tiles = gate_up.shape[0], downs.shape[0]

    def copies(i):
        cols = pl.ds(pl.multiple_of(i * tile, tile), tile)
        return (
            pltpu.make_async_copy(
                gate.at[:, cols], gate_up.at[i, :, pl.ds(0, tile)], sem_in.at[i, 0]
            ),
            pltpu.make_async_copy(
                up.at[:, cols], gate_up.at[i, :, pl.ds(tile, tile)], sem_in.at[i, 1]
            ),
        )

    def down_copy(j):
        return pltpu.make_async_copy(
            down.at[:, pl.ds(j * out_tile, out_tile)], downs.at[j], sem_down.at[j]
        )

    for i in range(tiles):
        for copy in copies(i):
            copy.start()
    for j in range(out_tiles):
        down_copy(j).start()
    at = 0
    for piece, size in zip(pieces, sizes):
        rows[at : at + size] = piece[...]
        at += size

    def first(i, carry):
        for copy in copies(i):
            copy.wait()
        both = jnp.dot(rows[...], gate_up[i], preferred_element_type=jnp.float32)
        gate_pre, up_pre = both[:, :tile], both[:, tile:]
        hidden[:, pl.ds(pl.multiple_of(i * tile, tile), tile)] = (
            jax.nn.silu(gate_pre) * up_pre
        ).astype(jnp.bfloat16)
        return carry

    lax.fori_loop(0, tiles, first, 0)
    for j in range(out_tiles):
        down_copy(j).wait()
        result = jnp.dot(hidden[...], downs[j], preferred_element_type=jnp.float32)
        result = result.astype(jnp.bfloat16)
        at = 0
        for out, size in zip(outs, sizes):
            out[:, j * out_tile : (j + 1) * out_tile] = result[at : at + size]
            at += size


def expert_rows(pieces, gate_part, up_part, down_part):
    features, width = gate_part.shape
    tile, out_tile = 128, 1024
    sizes = tuple(piece.shape[0] for piece in pieces)
    total = sum(sizes)
    here = pl.BlockSpec(memory_space=pltpu.VMEM)
    away = pl.BlockSpec(memory_space=pl.ANY)
    return pl.pallas_call(
        functools.partial(expert_kernel, sizes, tile, out_tile),
        out_shape=[jax.ShapeDtypeStruct((size, features), jnp.bfloat16) for size in sizes],
        in_specs=[here] * len(sizes) + [away] * 3,
        out_specs=[here] * len(sizes),
        scratch_shapes=[
            pltpu.VMEM((total, features), jnp.bfloat16),
            pltpu.VMEM((width // tile, features, 2 * tile), jnp.bfloat16),
            pltpu.VMEM((features // out_tile, width, out_tile), jnp.bfloat16),
            pltpu.VMEM((total, width), jnp.bfloat16),
            pltpu.SemaphoreType.DMA((width // tile, 2)),
            pltpu.SemaphoreType.DMA((features // out_tile,)),
        ],
        compiler_params=pltpu.CompilerParams(vmem_limit_bytes=40 * 2**20),
        cost_estimate=pl.CostEstimate(
            flops=6 * total * features * width,
            transcendentals=total * width,
            bytes_accessed=6 * features * width + 4 * total * features,
        ),
        name="expert_rows",
    )(*pieces, gate_part, up_part, down_part)


def added(one, other):
    return (one.astype(jnp.float32) + other.astype(jnp.float32)).astype(jnp.bfloat16)


def onward(value, back):
    sections = lax.axis_size("section")
    pairs = [
        (s * NZ + z, (s + 1) % sections * NZ + (z - back) % NZ)
        for s in range(sections)
        for z in range(NZ)
    ]
    return lax.ppermute(value, ("section", "wide_0"), pairs)


def homeward(number, o_own, to_left, to_right):
    from_left = passed_along(to_left, "wide_1", -1)
    from_right = passed_along(to_right, "wide_1", 1)
    summed = (
        o_own.astype(jnp.float32) + from_left.astype(jnp.float32) + from_right.astype(jnp.float32)
    ).astype(jnp.bfloat16)
    return {k: onward(summed[i * CAP : (i + 1) * CAP], k) for i, k in enumerate(CHUNKS[number])}


def expert_layer(residual, ffn_gain, router_weight, id_rows, gate_part, up_part, down_part):
    tok_rows = residual.shape[0]
    features = residual.shape[1]
    zi = lax.axis_index("wide_0")
    slots = route_slots(id_rows).reshape(tok_rows, TOP)
    routed = rms_scale(residual, ffn_gain).astype(jnp.bfloat16)
    logits = jnp.dot(routed, router_weight, preferred_element_type=jnp.float32)
    chosen = jnp.take_along_axis(logits, id_rows, axis=1)
    first_share = jax.nn.sigmoid(chosen[:, 0] - chosen[:, 1])
    shares = jnp.stack([first_share, 1.0 - first_share], axis=1)

    col_expert = ((zi + lax.broadcasted_iota(jnp.int32, (NZ, CAP), 0)) % NZ // 2).reshape(-1)
    col_slot = lax.broadcasted_iota(jnp.int32, (NZ, CAP), 1).reshape(-1)
    hits = [
        (id_rows[:, k][:, None] == col_expert[None, :]) & (slots[:, k][:, None] == col_slot[None, :])
        for k in range(TOP)
    ]
    placing = (hits[0] | hits[1]).astype(jnp.bfloat16)
    combine = jnp.where(hits[0], shares[:, 0:1], 0.0) + jnp.where(hits[1], shares[:, 1:2], 0.0)
    packed = lax.dot_general(
        placing, routed, (((0,), (0,)), ((), ())), preferred_element_type=jnp.float32
    ).astype(jnp.bfloat16).reshape(NZ, CAP, features)

    arrived = {}
    for chunk in CHUNKS:
        for k in chunk:
            arrived[k] = packed[0] if k == 0 else passed_along(packed[k], "wide_0", k)
    kept = jnp.concatenate(
        [residual, combine, jnp.zeros((tok_rows, 64), jnp.float32)], axis=1
    )

    answers = {}
    ahead = None
    for number, chunk in enumerate(CHUNKS):
        own = jnp.concatenate([arrived[k] for k in chunk], axis=0)
        if ahead is None:
            own, kept = lax.optimization_barrier((own, kept))
            kept = onward(kept, 0)
        half = own.shape[0] // 2
        left = passed_along(own, "wide_1", 1)
        right = passed_along(own, "wide_1", -1)
        far_a = passed_along(left[:half], "wide_1", 1)
        far_b = passed_along(right[half:], "wide_1", -1)
        if ahead is not None:
            far_b, ahead = lax.optimization_barrier((far_b, ahead))
            answers.update(homeward(number - 1, *ahead))
        o_own, o_left, o_right, o_far_a, o_far_b = expert_rows(
            (own, left, right, far_a, far_b), gate_part, up_part, down_part
        )
        mid_a = passed_along(o_far_a, "wide_1", -1)
        mid_b = passed_along(o_far_b, "wide_1", 1)
        to_left = jnp.concatenate([added(o_left[:half], mid_a), o_left[half:]], axis=0)
        to_right = jnp.concatenate([o_right[:half], added(o_right[half:], mid_b)], axis=0)
        ahead = (o_own, to_left, to_right)
    answers.update(homeward(len(CHUNKS) - 1, *ahead))
    stacked = jnp.concatenate([answers[k] for k in range(NZ)], axis=0)
    residual = kept[:, :features]
    combine = kept[:, features : features + NZ * CAP]
    combine_hi = lax.reduce_precision(combine, 8, 7)
    combine_lo = combine - combine_hi
    mixed_out = jnp.dot(
        combine_hi.astype(jnp.bfloat16), stacked, preferred_element_type=jnp.float32
    ) + jnp.dot(combine_lo.astype(jnp.bfloat16), stacked, preferred_element_type=jnp.float32)
    return (residual + mixed_out).astype(jnp.bfloat16)


def local(
    stream,
    mixer_gain,
    ssm_weight,
    decay_rate,
    skip_gain,
    mixed_gain,
    ffn_gain,
    router_weight,
    expert_ids,
    gate_weight,
    up_weight,
    down_weight,
):
    residual = mixer_block(
        stream[0], mixer_gain[0], ssm_weight[0], decay_rate[0], skip_gain[0], mixed_gain[0]
    )
    finished = expert_layer(
        residual,
        ffn_gain[0],
        router_weight[0],
        expert_ids[0],
        gate_weight[0],
        up_weight[0],
        down_weight[0],
    )
    return finished[None]


def solution(mesh):
    finer = Mesh(
        mesh.devices.reshape(mesh.shape["section"], NZ, NY), ("section", "wide_0", "wide_1")
    )
    placed = (
        P("section", WIDE, None),
        P("section", None),
        P("section", None, None),
        P("section", None),
        P("section", None),
        P("section", None),
        P("section", None),
        P("section", None, None),
        P("section", WIDE, None),
        P("section", None, WIDE),
        P("section", None, WIDE),
        P("section", WIDE, None),
    )
    return jax.shard_map(
        local, mesh=finer, in_specs=placed, out_specs=P("section", WIDE, None), check_vma=False
    )
```

```python
import functools
import math

import jax
import jax.numpy as jnp
from jax import lax
from jax.experimental import pallas as pl
from jax.experimental.pallas import tpu as pltpu
from jax.sharding import Mesh
from jax.sharding import PartitionSpec as P

HEADS = 32
HEAD_DIM = 64
STATE = 64
EXPERTS = 4
TOP = 2
CAP = 40
NZ = 8
NY = 4
WIDE = ("wide_0", "wide_1")
EPSILON = 1e-05
CHUNKS = ((0, 1, 7, 4), (2, 6, 3, 5))


def passed_along(value, axis, by):
    length = lax.axis_size(axis)
    return lax.ppermute(value, axis, [(i, (i + by) % length) for i in range(length)])


def rms_scale(values, gain_row):
    mean_sq = jnp.mean(values * values, axis=-1, keepdims=True)
    return values * lax.rsqrt(mean_sq + EPSILON) * gain_row


def route_slots(id_rows):
    flat_ids = id_rows.reshape(-1)
    one_hot = (
        flat_ids[:, None] == lax.broadcasted_iota(jnp.int32, (flat_ids.shape[0], EXPERTS), 1)
    ).astype(jnp.int32)
    running = jnp.cumsum(one_hot, axis=0) - 1
    slot_ids = jnp.sum(one_hot * running, axis=1)
    return slot_ids


def prefix_kernel(arrived_ref, out_ref):
    def step(k, carry):
        out_ref[k] = carry.astype(jnp.bfloat16)
        block = arrived_ref[k].astype(jnp.float32)
        decay = block[32:33] + block[33:34] + block[34:35]
        return carry * decay + block[:32]

    lax.fori_loop(0, NZ * NY, step, jnp.zeros((32, 128), jnp.float32))


def prefix_states(arrived):
    return pl.pallas_call(
        prefix_kernel,
        out_shape=jax.ShapeDtypeStruct((NZ * NY, 32, 128), jnp.bfloat16),
        in_specs=[pl.BlockSpec(memory_space=pltpu.VMEM)],
        out_specs=pl.BlockSpec(memory_space=pltpu.VMEM),
        name="prefix_states",
    )(arrived)


def carried_states(payload):
    arrived = lax.all_to_all(payload, WIDE, split_axis=0, concat_axis=0, tiled=True)
    back = lax.all_to_all(
        prefix_states(arrived), WIDE, split_axis=0, concat_axis=0, tiled=True
    )
    return back.reshape(16, 2, 32, 128).transpose(1, 2, 0, 3).reshape(STATE, -1)


def head_column(values, head):
    lanes = lax.broadcasted_iota(jnp.int32, values.shape, 1)
    return jnp.sum(jnp.where(lanes == head, values, 0.0), axis=1, keepdims=True)


def pair_columns(values, pair):
    shape = (values.shape[0], 2 * HEAD_DIM)
    lanes = lax.broadcasted_iota(jnp.int32, shape, 1)
    return jnp.where(
        lanes < HEAD_DIM, head_column(values, 2 * pair), head_column(values, 2 * pair + 1)
    )


def ordered(seq_len):
    rows = lax.broadcasted_iota(jnp.int32, (seq_len, seq_len), 0)
    return rows >= lax.broadcasted_iota(jnp.int32, (seq_len, seq_len), 1)


def front_kernel(
    inputs_ref, gain_ref, ssm_ref, rate_ref, payload_ref, normed_ref, maps_ref, step_ref, cum_ref
):
    values = inputs_ref[...].astype(jnp.float32)
    normed = rms_scale(values, gain_ref[...]).astype(jnp.bfloat16)
    normed_ref[...] = normed
    projected = lax.dot_general(
        normed, ssm_ref[...], (((1,), (1,)), ((), ())), preferred_element_type=jnp.float32
    )
    maps_ref[...] = projected[:, : 2 * STATE]
    raw = projected[:, 2 * STATE :]
    step_size = jnp.maximum(raw, 0.0) + jnp.log1p(jnp.exp(-jnp.abs(raw)))
    step_ref[...] = step_size
    seq_len = values.shape[0]
    cumulative = jnp.dot(
        ordered(seq_len).astype(jnp.float32),
        -step_size * rate_ref[...],
        precision=lax.Precision.HIGHEST,
        preferred_element_type=jnp.float32,
    )
    cum_ref[...] = cumulative
    total = cumulative[seq_len - 1 :]
    tail = jnp.exp(total - cumulative) * step_size
    decay = jnp.exp(total)
    b_rows = (projected[:, :STATE] / float(STATE)).astype(jnp.bfloat16)
    row = lax.broadcasted_iota(jnp.int32, (8, 2 * HEAD_DIM), 0)

    def pair_step(pair, carry):
        lanes = pl.ds(pl.multiple_of(pair * 2 * HEAD_DIM, 2 * HEAD_DIM), 2 * HEAD_DIM)
        here = normed_ref[:, lanes].astype(jnp.float32)
        weighted = (pair_columns(tail, pair) * here).astype(jnp.bfloat16)
        state = lax.dot_general(
            b_rows, weighted, (((0,), (0,)), ((), ())), preferred_element_type=jnp.float32
        )
        cols = pair_columns(decay, pair)
        high = cols.astype(jnp.bfloat16).astype(jnp.float32)
        mid = (cols - high).astype(jnp.bfloat16).astype(jnp.float32)
        low = cols - high - mid
        extra = jnp.where(
            row == 0, high, jnp.where(row == 1, mid, jnp.where(row == 2, low, 0.0))
        )
        for half in range(2):
            block = jnp.concatenate([state[half * 32 : half * 32 + 32], extra], axis=0)
            payload_ref[2 * pair + half] = block.astype(jnp.bfloat16)
        return carry

    lax.fori_loop(0, HEADS // 2, pair_step, 0)


def within_kernel(normed_ref, maps_ref, step_ref, cum_ref, skip_ref, out_ref, cum_t, step_t):
    cumulative = cum_ref[...]
    cum_t[...] = cumulative.T
    step_t[...] = step_ref[...].T
    seq_len = cumulative.shape[0]
    mask = ordered(seq_len)
    b_rows = (maps_ref[:, :STATE] / float(STATE)).astype(jnp.bfloat16)
    c_rows = (maps_ref[:, STATE:] / math.sqrt(STATE)).astype(jnp.bfloat16)
    meets = lax.dot_general(
        c_rows, b_rows, (((1,), (1,)), ((), ())), preferred_element_type=jnp.float32
    )

    def pair_step(pair, carry):
        lanes = pl.ds(pl.multiple_of(pair * 2 * HEAD_DIM, 2 * HEAD_DIM), 2 * HEAD_DIM)
        here = normed_ref[:, lanes]
        results = []
        for side in range(2):
            head = 2 * pair + side
            gaps = head_column(cumulative, head) - cum_t[pl.ds(head, 1), :]
            kernel = jnp.where(mask, jnp.exp(jnp.where(mask, gaps, 0.0)), 0.0)
            mixing = (meets * kernel * step_t[pl.ds(head, 1), :]).astype(jnp.bfloat16)
            results.append(jnp.dot(mixing, here, preferred_element_type=jnp.float32))
        left = lax.broadcasted_iota(jnp.int32, results[0].shape, 1) < HEAD_DIM
        skip = pair_columns(skip_ref[...], pair)
        out_ref[:, lanes] = (
            jnp.where(left, results[0], results[1]) + here.astype(jnp.float32) * skip
        )
        return carry

    lax.fori_loop(0, HEADS // 2, pair_step, 0)


def mixer_block(inputs, mixer_gain, ssm_weight, decay_rate, skip_gain, mixed_gain):
    seq_len, features = inputs.shape
    here = pl.BlockSpec(memory_space=pltpu.VMEM)
    payload, normed, maps, step_size, cumulative = pl.pallas_call(
        front_kernel,
        out_shape=[
            jax.ShapeDtypeStruct((NZ * NY, 40, 2 * HEAD_DIM), jnp.bfloat16),
            jax.ShapeDtypeStruct((seq_len, features), jnp.bfloat16),
            jax.ShapeDtypeStruct((seq_len, 2 * STATE), jnp.float32),
            jax.ShapeDtypeStruct((seq_len, HEADS), jnp.float32),
            jax.ShapeDtypeStruct((seq_len, HEADS), jnp.float32),
        ],
        in_specs=[here] * 4,
        out_specs=[here] * 5,
        name="front",
    )(inputs, mixer_gain[None], ssm_weight.T, decay_rate[None])
    carried_in = carried_states(payload)
    within = pl.pallas_call(
        within_kernel,
        out_shape=jax.ShapeDtypeStruct((seq_len, features), jnp.float32),
        in_specs=[here] * 5,
        out_specs=here,
        scratch_shapes=[
            pltpu.VMEM((HEADS, seq_len), jnp.float32),
            pltpu.VMEM((HEADS, seq_len), jnp.float32),
        ],
        cost_estimate=pl.CostEstimate(
            flops=10 * seq_len * seq_len * features,
            transcendentals=seq_len * seq_len * HEADS,
            bytes_accessed=8 * seq_len * features,
        ),
        name="within",
    )(normed, maps, step_size, cumulative, skip_gain[None])
    c_rows = maps[:, STATE:] / math.sqrt(STATE)
    carried_part = jnp.dot(
        c_rows.astype(jnp.bfloat16), carried_in, preferred_element_type=jnp.float32
    ) * jnp.repeat(jnp.exp(cumulative), HEAD_DIM, axis=1)
    return inputs.astype(jnp.float32) + rms_scale(within + carried_part, mixed_gain)


def expert_kernel(sizes, tile, out_tile, *refs):
    n = len(sizes)
    pieces, (gate, up, down), outs = refs[:n], refs[n : n + 3], refs[n + 3 : 2 * n + 3]
    rows, gate_up, downs, hidden, sem_in, sem_down = refs[2 * n + 3 :]
    tiles, out_tiles = gate_up.shape[0], downs.shape[0]

    def copies(i):
        cols = pl.ds(pl.multiple_of(i * tile, tile), tile)
        return (
            pltpu.make_async_copy(
                gate.at[:, cols], gate_up.at[i, :, pl.ds(0, tile)], sem_in.at[i, 0]
            ),
            pltpu.make_async_copy(
                up.at[:, cols], gate_up.at[i, :, pl.ds(tile, tile)], sem_in.at[i, 1]
            ),
        )

    def down_copy(j):
        return pltpu.make_async_copy(
            down.at[:, pl.ds(pl.multiple_of(j * out_tile, out_tile), out_tile)],
            downs.at[j],
            sem_down.at[j],
        )

    for i in range(tiles):
        for copy in copies(i):
            copy.start()
    for j in range(out_tiles):
        down_copy(j).start()
    at = 0
    for piece, size in zip(pieces, sizes):

        def gather(i, carry, piece=piece, at=at):
            rows[pl.ds(pl.multiple_of(at + i * 16, 16), 16)] = piece[
                pl.ds(pl.multiple_of(i * 16, 16), 16)
            ]
            return carry

        lax.fori_loop(0, size // 16, gather, 0)
        at += size

    def first(i, carry):
        for copy in copies(i):
            copy.wait()
        both = jnp.dot(rows[...], gate_up[i], preferred_element_type=jnp.float32)
        gate_pre, up_pre = both[:, :tile], both[:, tile:]
        hidden[:, pl.ds(pl.multiple_of(i * tile, tile), tile)] = (
            jax.nn.silu(gate_pre) * up_pre
        ).astype(jnp.bfloat16)
        return carry

    lax.fori_loop(0, tiles, first, 0)

    def second(j, carry):
        down_copy(j).wait()
        result = jnp.dot(hidden[...], downs[j], preferred_element_type=jnp.float32)
        result = result.astype(jnp.bfloat16)
        at = 0
        for out, size in zip(outs, sizes):
            out[:, pl.ds(pl.multiple_of(j * out_tile, out_tile), out_tile)] = result[at : at + size]
            at += size
        return carry

    lax.fori_loop(0, out_tiles, second, 0)


def expert_rows(pieces, gate_part, up_part, down_part):
    features, width = gate_part.shape
    tile, out_tile = 128, 512
    sizes = tuple(piece.shape[0] for piece in pieces)
    total = sum(sizes)
    here = pl.BlockSpec(memory_space=pltpu.VMEM)
    away = pl.BlockSpec(memory_space=pltpu.HBM)
    return pl.pallas_call(
        functools.partial(expert_kernel, sizes, tile, out_tile),
        out_shape=[jax.ShapeDtypeStruct((size, features), jnp.bfloat16) for size in sizes],
        in_specs=[here] * len(sizes) + [away] * 3,
        out_specs=[here] * len(sizes),
        scratch_shapes=[
            pltpu.VMEM((total, features), jnp.bfloat16),
            pltpu.VMEM((width // tile, features, 2 * tile), jnp.bfloat16),
            pltpu.VMEM((features // out_tile, width, out_tile), jnp.bfloat16),
            pltpu.VMEM((total, width), jnp.bfloat16),
            pltpu.SemaphoreType.DMA((width // tile, 2)),
            pltpu.SemaphoreType.DMA((features // out_tile,)),
        ],
        compiler_params=pltpu.CompilerParams(vmem_limit_bytes=40 * 2**20),
        cost_estimate=pl.CostEstimate(
            flops=6 * total * features * width,
            transcendentals=total * width,
            bytes_accessed=6 * features * width + 4 * total * features,
        ),
        name="expert_rows",
    )(*pieces, gate_part, up_part, down_part)


def join_kernel(*refs):
    blocks, out = refs[:-1], refs[-1]
    rows = blocks[0].shape[0]
    for number, block in enumerate(blocks):

        def copy(i, carry, block=block, at=number * rows):
            out[pl.ds(pl.multiple_of(at + i * 8, 8), 8)] = block[pl.ds(pl.multiple_of(i * 8, 8), 8)]
            return carry

        lax.fori_loop(0, rows // 8, copy, 0)


def joined(blocks):
    rows, features = blocks[0].shape
    here = pl.BlockSpec(memory_space=pltpu.VMEM)
    return pl.pallas_call(
        join_kernel,
        out_shape=jax.ShapeDtypeStruct((rows * len(blocks), features), blocks[0].dtype),
        in_specs=[here] * len(blocks),
        out_specs=here,
        name="join",
    )(*blocks)


def added(one, other):
    return (one.astype(jnp.float32) + other.astype(jnp.float32)).astype(jnp.bfloat16)


def onward(value, back):
    sections = lax.axis_size("section")
    pairs = [
        (s * NZ + z, (s + 1) % sections * NZ + (z - back) % NZ)
        for s in range(sections)
        for z in range(NZ)
    ]
    return lax.ppermute(value, ("section", "wide_0"), pairs)


def homeward(number, o_own, to_left, to_right):
    from_left = passed_along(to_left, "wide_1", -1)
    from_right = passed_along(to_right, "wide_1", 1)
    summed = (
        o_own.astype(jnp.float32) + from_left.astype(jnp.float32) + from_right.astype(jnp.float32)
    ).astype(jnp.bfloat16)
    return {k: summed[i * CAP : (i + 1) * CAP] for i, k in enumerate(CHUNKS[number])}


def weighted_rows(weights, rows):
    high = lax.reduce_precision(weights, 8, 7)
    both = [high.astype(jnp.bfloat16), (weights - high).astype(jnp.bfloat16)]
    return sum(jnp.dot(part, rows, preferred_element_type=jnp.float32) for part in both)


def expert_layer(residual, ffn_gain, router_weight, id_rows, gate_part, up_part, down_part):
    tok_rows = residual.shape[0]
    features = residual.shape[1]
    zi = lax.axis_index("wide_0")
    slots = route_slots(id_rows).reshape(tok_rows, TOP)
    routed = rms_scale(residual, ffn_gain).astype(jnp.bfloat16)
    logits = jnp.dot(routed, router_weight, preferred_element_type=jnp.float32)
    experts = lax.broadcasted_iota(jnp.int32, (tok_rows, EXPERTS), 1)
    signs = (experts == id_rows[:, :1]).astype(jnp.float32) - (
        experts == id_rows[:, 1:]
    ).astype(jnp.float32)
    first_share = jax.nn.sigmoid(jnp.sum(logits * signs, axis=1))
    shares = jnp.stack([first_share, 1.0 - first_share], axis=1)

    col_expert = ((zi + lax.broadcasted_iota(jnp.int32, (NZ, CAP), 0)) % NZ // 2).reshape(-1)
    col_slot = lax.broadcasted_iota(jnp.int32, (NZ, CAP), 1).reshape(-1)
    hits = [
        (id_rows[:, k][:, None] == col_expert[None, :]) & (slots[:, k][:, None] == col_slot[None, :])
        for k in range(TOP)
    ]
    placing = (hits[0] | hits[1]).astype(jnp.bfloat16)
    combine = jnp.where(hits[0], shares[:, 0:1], 0.0) + jnp.where(hits[1], shares[:, 1:2], 0.0)
    packed = lax.dot_general(
        placing, routed, (((0,), (0,)), ((), ())), preferred_element_type=jnp.float32
    ).astype(jnp.bfloat16).reshape(NZ, CAP, features)

    arrived = {}
    for chunk in CHUNKS:
        for k in chunk:
            arrived[k] = packed[0] if k == 0 else passed_along(packed[k], "wide_0", k)
    answers, kept = {}, []

    def finish(number, *sums):
        for k, block in homeward(number, *sums).items():
            if k:
                answers[k] = onward(block, k)
                continue
            own_part = residual + weighted_rows(combine[:, :CAP], block)
            wide = jnp.concatenate(
                [own_part, combine[:, CAP:], jnp.zeros((tok_rows, 104), jnp.float32)], axis=1
            )
            kept.append(onward(wide, 0))

    ahead = None
    for number, chunk in enumerate(CHUNKS):
        own = joined([arrived[k] for k in chunk])
        half = own.shape[0] // 2
        left = passed_along(own, "wide_1", 1)
        right = passed_along(own, "wide_1", -1)
        far_a = passed_along(left[:half], "wide_1", 1)
        far_b = passed_along(right[half:], "wide_1", -1)
        if ahead is not None:
            finish(number - 1, *ahead)
        o_own, o_left, o_right, o_far_a, o_far_b = expert_rows(
            (own, left, right, far_a, far_b), gate_part, up_part, down_part
        )
        mid_a = passed_along(o_far_a, "wide_1", -1)
        mid_b = passed_along(o_far_b, "wide_1", 1)
        to_left = jnp.concatenate([added(o_left[:half], mid_a), o_left[half:]], axis=0)
        to_right = jnp.concatenate([o_right[:half], added(o_right[half:], mid_b)], axis=0)
        ahead = (o_own, to_left, to_right)
    finish(len(CHUNKS) - 1, *ahead)
    stacked = joined([answers[k] for k in range(1, NZ)])
    kept = kept[0]
    rest = kept[:, features : features + (NZ - 1) * CAP]
    return (kept[:, :features] + weighted_rows(rest, stacked)).astype(jnp.bfloat16)


def local(
    stream,
    mixer_gain,
    ssm_weight,
    decay_rate,
    skip_gain,
    mixed_gain,
    ffn_gain,
    router_weight,
    expert_ids,
    gate_weight,
    up_weight,
    down_weight,
):
    residual = mixer_block(
        stream[0], mixer_gain[0], ssm_weight[0], decay_rate[0], skip_gain[0], mixed_gain[0]
    )
    finished = expert_layer(
        residual,
        ffn_gain[0],
        router_weight[0],
        expert_ids[0],
        gate_weight[0],
        up_weight[0],
        down_weight[0],
    )
    return finished[None]


def solution(mesh):
    finer = Mesh(
        mesh.devices.reshape(mesh.shape["section"], NZ, NY), ("section", "wide_0", "wide_1")
    )
    placed = (
        P("section", WIDE, None),
        P("section", None),
        P("section", None, None),
        P("section", None),
        P("section", None),
        P("section", None),
        P("section", None),
        P("section", None, None),
        P("section", WIDE, None),
        P("section", None, WIDE),
        P("section", None, WIDE),
        P("section", WIDE, None),
    )
    return jax.shard_map(
        local, mesh=finer, in_specs=placed, out_specs=P("section", WIDE, None), check_vma=False
    )
```

```python
import functools
import math

import jax
import jax.numpy as jnp
from jax import lax
from jax.experimental import pallas as pl
from jax.experimental.pallas import tpu as pltpu
from jax.sharding import Mesh
from jax.sharding import PartitionSpec as P

HEADS = 32
HEAD_DIM = 64
STATE = 64
EXPERTS = 4
TOP = 2
CAP = 40
NZ = 8
NY = 4
WIDE = ("wide_0", "wide_1")
EPSILON = 1e-05
SHIFTS = (0, 2, 6, 4)


def along_y(value, by):
    return lax.ppermute(value, "wide_1", [(y, (y + by) % NY) for y in range(NY)])


def along_z(value, target):
    return lax.ppermute(value, "wide_0", [(z, target(z) % NZ) for z in range(NZ)])


def rms_scale(values, gain_row):
    mean_sq = jnp.mean(values * values, axis=-1, keepdims=True)
    return values * lax.rsqrt(mean_sq + EPSILON) * gain_row


def route_slots(id_rows):
    flat_ids = id_rows.reshape(-1)
    one_hot = (
        flat_ids[:, None] == lax.broadcasted_iota(jnp.int32, (flat_ids.shape[0], EXPERTS), 1)
    ).astype(jnp.int32)
    running = jnp.cumsum(one_hot, axis=0) - 1
    slot_ids = jnp.sum(one_hot * running, axis=1)
    return slot_ids


def prefix_kernel(arrived_ref, out_ref):
    def step(k, carry):
        out_ref[k] = carry.astype(jnp.bfloat16)
        block = arrived_ref[k].astype(jnp.float32)
        decay = block[32:33] + block[33:34] + block[34:35]
        return carry * decay + block[:32]

    lax.fori_loop(0, NZ * NY, step, jnp.zeros((32, 128), jnp.float32), unroll=8)


def prefix_states(arrived):
    return pl.pallas_call(
        prefix_kernel,
        out_shape=jax.ShapeDtypeStruct((NZ * NY, 32, 128), jnp.bfloat16),
        in_specs=[pl.BlockSpec(memory_space=pltpu.VMEM)],
        out_specs=pl.BlockSpec(memory_space=pltpu.VMEM),
        name="prefix_states",
    )(pltpu.with_memory_space_constraint(arrived, pltpu.VMEM))


def carried_states(payload):
    arrived = lax.all_to_all(payload, WIDE, split_axis=0, concat_axis=0, tiled=True)
    back = lax.all_to_all(
        prefix_states(arrived), WIDE, split_axis=0, concat_axis=0, tiled=True
    )
    return back.reshape(16, 2, 32, 128).transpose(1, 2, 0, 3).reshape(STATE, -1)


def head_column(values, head):
    lanes = lax.broadcasted_iota(jnp.int32, values.shape, 1)
    return jnp.sum(jnp.where(lanes == head, values, 0.0), axis=1, keepdims=True)


def pair_columns(values, pair):
    shape = (values.shape[0], 2 * HEAD_DIM)
    lanes = lax.broadcasted_iota(jnp.int32, shape, 1)
    return jnp.where(
        lanes < HEAD_DIM, head_column(values, 2 * pair), head_column(values, 2 * pair + 1)
    )


def ordered(seq_len):
    rows = lax.broadcasted_iota(jnp.int32, (seq_len, seq_len), 0)
    return rows >= lax.broadcasted_iota(jnp.int32, (seq_len, seq_len), 1)


def front_kernel(
    inputs_ref, gain_ref, ssm_ref, rate_ref, payload_ref, normed_ref, maps_ref, step_ref, cum_ref
):
    values = inputs_ref[...].astype(jnp.float32)
    normed = rms_scale(values, gain_ref[...]).astype(jnp.bfloat16)
    normed_ref[...] = normed
    projected = lax.dot_general(
        normed, ssm_ref[...], (((1,), (1,)), ((), ())), preferred_element_type=jnp.float32
    )
    maps_ref[...] = projected[:, : 2 * STATE]
    raw = projected[:, 2 * STATE :]
    step_size = jnp.maximum(raw, 0.0) + jnp.log1p(jnp.exp(-jnp.abs(raw)))
    step_ref[...] = step_size
    seq_len = values.shape[0]
    cumulative = jnp.dot(
        ordered(seq_len).astype(jnp.float32),
        -step_size * rate_ref[...],
        precision=lax.Precision.HIGHEST,
        preferred_element_type=jnp.float32,
    )
    cum_ref[...] = cumulative
    total = cumulative[seq_len - 1 :]
    tail = jnp.exp(total - cumulative) * step_size
    decay = jnp.exp(total)
    b_rows = (projected[:, :STATE] / float(STATE)).astype(jnp.bfloat16)
    row = lax.broadcasted_iota(jnp.int32, (8, 2 * HEAD_DIM), 0)

    def pair_step(pair, carry):
        lanes = pl.ds(pl.multiple_of(pair * 2 * HEAD_DIM, 2 * HEAD_DIM), 2 * HEAD_DIM)
        here = normed_ref[:, lanes].astype(jnp.float32)
        weighted = (pair_columns(tail, pair) * here).astype(jnp.bfloat16)
        state = lax.dot_general(
            b_rows, weighted, (((0,), (0,)), ((), ())), preferred_element_type=jnp.float32
        )
        cols = pair_columns(decay, pair)
        high = cols.astype(jnp.bfloat16).astype(jnp.float32)
        mid = (cols - high).astype(jnp.bfloat16).astype(jnp.float32)
        low = cols - high - mid
        extra = jnp.where(
            row == 0, high, jnp.where(row == 1, mid, jnp.where(row == 2, low, 0.0))
        )
        for half in range(2):
            block = jnp.concatenate([state[half * 32 : half * 32 + 32], extra], axis=0)
            payload_ref[2 * pair + half] = block.astype(jnp.bfloat16)
        return carry

    lax.fori_loop(0, HEADS // 2, pair_step, 0, unroll=4)


def within_kernel(normed_ref, maps_ref, step_ref, cum_ref, skip_ref, out_ref, cum_t, step_t):
    cumulative = cum_ref[...]
    cum_t[...] = cumulative.T
    step_t[...] = step_ref[...].T
    seq_len = cumulative.shape[0]
    mask = ordered(seq_len)
    b_rows = (maps_ref[:, :STATE] / float(STATE)).astype(jnp.bfloat16)
    c_rows = (maps_ref[:, STATE:] / math.sqrt(STATE)).astype(jnp.bfloat16)
    meets = lax.dot_general(
        c_rows, b_rows, (((1,), (1,)), ((), ())), preferred_element_type=jnp.float32
    )

    def pair_step(pair, carry):
        lanes = pl.ds(pl.multiple_of(pair * 2 * HEAD_DIM, 2 * HEAD_DIM), 2 * HEAD_DIM)
        here = normed_ref[:, lanes]
        results = []
        for side in range(2):
            head = 2 * pair + side
            gaps = head_column(cumulative, head) - cum_t[pl.ds(head, 1), :]
            kernel = jnp.where(mask, jnp.exp(jnp.where(mask, gaps, 0.0)), 0.0)
            mixing = (meets * kernel * step_t[pl.ds(head, 1), :]).astype(jnp.bfloat16)
            results.append(jnp.dot(mixing, here, preferred_element_type=jnp.float32))
        left = lax.broadcasted_iota(jnp.int32, results[0].shape, 1) < HEAD_DIM
        skip = pair_columns(skip_ref[...], pair)
        out_ref[:, lanes] = (
            jnp.where(left, results[0], results[1]) + here.astype(jnp.float32) * skip
        )
        return carry

    lax.fori_loop(0, HEADS // 2, pair_step, 0)


def mixer_block(inputs, mixer_gain, ssm_weight, decay_rate, skip_gain, mixed_gain):
    seq_len, features = inputs.shape
    here = pl.BlockSpec(memory_space=pltpu.VMEM)
    payload, normed, maps, step_size, cumulative = pl.pallas_call(
        front_kernel,
        out_shape=[
            jax.ShapeDtypeStruct((NZ * NY, 40, 2 * HEAD_DIM), jnp.bfloat16),
            jax.ShapeDtypeStruct((seq_len, features), jnp.bfloat16),
            jax.ShapeDtypeStruct((seq_len, 2 * STATE), jnp.float32),
            jax.ShapeDtypeStruct((seq_len, HEADS), jnp.float32),
            jax.ShapeDtypeStruct((seq_len, HEADS), jnp.float32),
        ],
        in_specs=[here] * 4,
        out_specs=[here] * 5,
        name="front",
    )(inputs, mixer_gain[None], ssm_weight.T, decay_rate[None])
    carried_in = carried_states(payload)
    within = pl.pallas_call(
        within_kernel,
        out_shape=jax.ShapeDtypeStruct((seq_len, features), jnp.float32),
        in_specs=[here] * 5,
        out_specs=here,
        scratch_shapes=[
            pltpu.VMEM((HEADS, seq_len), jnp.float32),
            pltpu.VMEM((HEADS, seq_len), jnp.float32),
        ],
        cost_estimate=pl.CostEstimate(
            flops=10 * seq_len * seq_len * features,
            transcendentals=seq_len * seq_len * HEADS,
            bytes_accessed=8 * seq_len * features,
        ),
        name="within",
    )(normed, maps, step_size, cumulative, skip_gain[None])
    c_rows = maps[:, STATE:] / math.sqrt(STATE)
    carried_part = jnp.dot(
        c_rows.astype(jnp.bfloat16), carried_in, preferred_element_type=jnp.float32
    ) * jnp.repeat(jnp.exp(cumulative), HEAD_DIM, axis=1)
    return inputs.astype(jnp.float32) + rms_scale(within + carried_part, mixed_gain)


def expert_kernel(sizes, tile, out_tile, *refs):
    n = len(sizes)
    pieces, (gate, up, down), outs = refs[:n], refs[n : n + 3], refs[n + 3 : 2 * n + 3]
    rows, gate_up, downs, hidden, sem_in, sem_down = refs[2 * n + 3 :]
    tiles, out_tiles = gate_up.shape[0], downs.shape[0]

    def copies(i):
        cols = pl.ds(pl.multiple_of(i * tile, tile), tile)
        return (
            pltpu.make_async_copy(
                gate.at[:, cols], gate_up.at[i, :, pl.ds(0, tile)], sem_in.at[i, 0]
            ),
            pltpu.make_async_copy(
                up.at[:, cols], gate_up.at[i, :, pl.ds(tile, tile)], sem_in.at[i, 1]
            ),
        )

    def down_copy(j):
        return pltpu.make_async_copy(
            down.at[:, pl.ds(pl.multiple_of(j * out_tile, out_tile), out_tile)],
            downs.at[j],
            sem_down.at[j],
        )

    for i in range(tiles):
        for copy in copies(i):
            copy.start()
    for j in range(out_tiles):
        down_copy(j).start()
    at = 0
    for piece, size in zip(pieces, sizes):

        def gather(i, carry, piece=piece, at=at):
            rows[pl.ds(pl.multiple_of(at + i * 16, 16), 16)] = piece[
                pl.ds(pl.multiple_of(i * 16, 16), 16)
            ]
            return carry

        lax.fori_loop(0, size // 16, gather, 0)
        at += size

    def first(i, carry):
        for copy in copies(i):
            copy.wait()
        both = jnp.dot(rows[...], gate_up[i], preferred_element_type=jnp.float32)
        gate_pre, up_pre = both[:, :tile], both[:, tile:]
        hidden[:, pl.ds(pl.multiple_of(i * tile, tile), tile)] = (
            jax.nn.silu(gate_pre) * up_pre
        ).astype(jnp.bfloat16)
        return carry

    lax.fori_loop(0, tiles, first, 0)

    def second(j, carry):
        down_copy(j).wait()
        result = jnp.dot(hidden[...], downs[j], preferred_element_type=jnp.float32)
        result = result.astype(jnp.bfloat16)
        at = 0
        for out, size in zip(outs, sizes):
            out[:, pl.ds(pl.multiple_of(j * out_tile, out_tile), out_tile)] = result[at : at + size]
            at += size
        return carry

    lax.fori_loop(0, out_tiles, second, 0)


def expert_rows(pieces, *weights):
    features, width = weights[0].shape
    tile, out_tile = 128, 512
    sizes = tuple(piece.shape[0] for piece in pieces)
    total = sum(sizes)
    here = pl.BlockSpec(memory_space=pltpu.VMEM)
    away = pl.BlockSpec(memory_space=pltpu.HBM)
    return pl.pallas_call(
        functools.partial(expert_kernel, sizes, tile, out_tile),
        out_shape=[jax.ShapeDtypeStruct((size, features), jnp.bfloat16) for size in sizes],
        in_specs=[here] * len(sizes) + [away] * 3,
        out_specs=[here] * len(sizes),
        scratch_shapes=[
            pltpu.VMEM((total, features), jnp.bfloat16),
            pltpu.VMEM((width // tile, features, 2 * tile), jnp.bfloat16),
            pltpu.VMEM((features // out_tile, width, out_tile), jnp.bfloat16),
            pltpu.VMEM((total, width), jnp.bfloat16),
            pltpu.SemaphoreType.DMA((width // tile, 2)),
            pltpu.SemaphoreType.DMA((features // out_tile,)),
        ],
        compiler_params=pltpu.CompilerParams(vmem_limit_bytes=24 * 2**20),
        cost_estimate=pl.CostEstimate(
            flops=6 * total * features * width,
            transcendentals=total * width,
            bytes_accessed=6 * features * width + 4 * total * features,
        ),
        name="expert_rows",
    )(*pieces, *(pltpu.with_memory_space_constraint(w, pltpu.HBM) for w in weights))


def join_kernel(*refs):
    blocks, out = refs[:-1], refs[-1]
    rows = blocks[0].shape[0]
    for number, block in enumerate(blocks):

        def copy(i, carry, block=block, at=number * rows):
            out[pl.ds(pl.multiple_of(at + i * 8, 8), 8)] = block[pl.ds(pl.multiple_of(i * 8, 8), 8)]
            return carry

        lax.fori_loop(0, rows // 8, copy, 0)


def joined(blocks):
    rows, features = blocks[0].shape
    here = pl.BlockSpec(memory_space=pltpu.VMEM)
    return pl.pallas_call(
        join_kernel,
        out_shape=jax.ShapeDtypeStruct((rows * len(blocks), features), blocks[0].dtype),
        in_specs=[here] * len(blocks),
        out_specs=here,
        name="join",
    )(*(pltpu.with_memory_space_constraint(block, pltpu.VMEM) for block in blocks))


def added(one, other):
    return (one.astype(jnp.float32) + other.astype(jnp.float32)).astype(jnp.bfloat16)


def onward(value, target):
    sections = lax.axis_size("section")
    pairs = [
        (s * NZ + z, (s + 1) % sections * NZ + target(z) % NZ)
        for s in range(sections)
        for z in range(NZ)
    ]
    return lax.ppermute(value, ("section", "wide_0"), pairs)


def finish_kernel(kept_ref, *refs):
    answers, out_ref, stacked = refs[:-2], refs[-2], refs[-1]
    for number, answer in enumerate(answers):

        def copy(i, carry, answer=answer, at=number * CAP):
            stacked[pl.ds(pl.multiple_of(at + i * 8, 8), 8)] = answer[
                pl.ds(pl.multiple_of(i * 8, 8), 8)
            ]
            return carry

        lax.fori_loop(0, CAP // 8, copy, 0, unroll=True)
    features = out_ref.shape[1]
    weights = kept_ref[:, features : features + len(SHIFTS) * CAP]
    parts = [weights[:, :CAP]]
    for i in range(1, len(SHIFTS)):
        parts += [weights[:, i * CAP : (i + 1) * CAP]] * 2
    weights = jnp.concatenate(parts, axis=1)
    high = weights.astype(jnp.bfloat16)
    low = (weights - high.astype(jnp.float32)).astype(jnp.bfloat16)
    for at in range(0, features, 512):
        rows = stacked[:, at : at + 512]
        result = kept_ref[:, at : at + 512] + jnp.dot(
            high, rows, preferred_element_type=jnp.float32
        )
        result += jnp.dot(low, rows, preferred_element_type=jnp.float32)
        out_ref[:, at : at + 512] = result.astype(jnp.bfloat16)


def finished(kept, answers):
    rows, features = kept.shape[0], answers[0].shape[1]
    here = pl.BlockSpec(memory_space=pltpu.VMEM)
    return pl.pallas_call(
        finish_kernel,
        out_shape=jax.ShapeDtypeStruct((rows, features), jnp.bfloat16),
        in_specs=[here] * (1 + len(answers)),
        out_specs=here,
        scratch_shapes=[pltpu.VMEM((len(answers) * CAP, features), jnp.bfloat16)],
        name="finish",
    )(*(pltpu.with_memory_space_constraint(value, pltpu.VMEM) for value in (kept, *answers)))


def weighted_rows(weights, rows):
    high = lax.reduce_precision(weights, 8, 7)
    both = [high.astype(jnp.bfloat16), (weights - high).astype(jnp.bfloat16)]
    return sum(jnp.dot(part, rows, preferred_element_type=jnp.float32) for part in both)


def expert_layer(residual, ffn_gain, router_weight, id_rows, gate_part, up_part, down_part):
    tok_rows = residual.shape[0]
    features = residual.shape[1]
    zi = lax.axis_index("wide_0")
    slots = route_slots(id_rows).reshape(tok_rows, TOP)
    routed = rms_scale(residual, ffn_gain).astype(jnp.bfloat16)
    logits = jnp.dot(routed, router_weight, preferred_element_type=jnp.float32)
    experts = lax.broadcasted_iota(jnp.int32, (tok_rows, EXPERTS), 1)
    signs = (experts == id_rows[:, :1]).astype(jnp.float32) - (
        experts == id_rows[:, 1:]
    ).astype(jnp.float32)
    first_share = jax.nn.sigmoid(jnp.sum(logits * signs, axis=1))
    shares = jnp.stack([first_share, 1.0 - first_share], axis=1)

    shifts = [jnp.full((CAP,), shift, jnp.int32) for shift in SHIFTS]
    col_expert = (zi + jnp.concatenate(shifts)) % NZ // 2
    col_slot = lax.broadcasted_iota(jnp.int32, (len(SHIFTS), CAP), 1).reshape(-1)
    hits = [
        (id_rows[:, k][:, None] == col_expert[None, :]) & (slots[:, k][:, None] == col_slot[None, :])
        for k in range(TOP)
    ]
    placing = (hits[0] | hits[1]).astype(jnp.bfloat16)
    combine = jnp.where(hits[0], shares[:, 0:1], 0.0) + jnp.where(hits[1], shares[:, 1:2], 0.0)
    packed = lax.dot_general(
        placing, routed, (((0,), (0,)), ((), ())), preferred_element_type=jnp.float32
    ).astype(jnp.bfloat16).reshape(len(SHIFTS), CAP, features)

    blocks = [packed[0]]
    for shift, block in zip(SHIFTS[1:], packed[1:]):
        blocks.append(along_z(block, lambda z, by=shift: z + by))
    even = joined(blocks)
    odd = along_z(even, lambda z: z ^ 1)

    sums = []
    for own in (even, odd):
        half = own.shape[0] // 2
        left = along_y(own, 1)
        right = along_y(own, -1)
        far_a = along_y(left[:half], 1)
        far_b = along_y(right[half:], -1)
        o_own, o_left, o_right, o_far_a, o_far_b = expert_rows(
            (own, left, right, far_a, far_b), gate_part, up_part, down_part
        )
        mid_a = along_y(o_far_a, -1)
        mid_b = along_y(o_far_b, 1)
        to_left = jnp.concatenate([added(o_left[:half], mid_a), o_left[half:]], axis=0)
        to_right = jnp.concatenate([o_right[:half], added(o_right[half:], mid_b)], axis=0)
        from_left = along_y(to_left, -1)
        from_right = along_y(to_right, 1)
        total = o_own.astype(jnp.float32) + from_left.astype(jnp.float32)
        sums.append((total + from_right.astype(jnp.float32)).astype(jnp.bfloat16))

    own_part = residual + weighted_rows(combine[:, :CAP], sums[0][:CAP])
    spare = jnp.zeros((tok_rows, 96), jnp.float32)
    kept = onward(jnp.concatenate([own_part, combine, spare], axis=1), lambda z: z)
    answers = []
    for i, shift in enumerate(SHIFTS):
        part = slice(i * CAP, (i + 1) * CAP)
        if i:
            answers.append(onward(sums[0][part], lambda z, by=shift: z - by))
        answers.append(onward(sums[1][part], lambda z, by=shift: (z ^ 1) - by))
    return finished(kept, answers)


def local(
    stream,
    mixer_gain,
    ssm_weight,
    decay_rate,
    skip_gain,
    mixed_gain,
    ffn_gain,
    router_weight,
    expert_ids,
    gate_weight,
    up_weight,
    down_weight,
):
    residual = mixer_block(
        stream[0], mixer_gain[0], ssm_weight[0], decay_rate[0], skip_gain[0], mixed_gain[0]
    )
    result = expert_layer(
        residual,
        ffn_gain[0],
        router_weight[0],
        expert_ids[0],
        gate_weight[0],
        up_weight[0],
        down_weight[0],
    )
    return result[None]


def solution(mesh):
    finer = Mesh(
        mesh.devices.reshape(mesh.shape["section"], NZ, NY), ("section", "wide_0", "wide_1")
    )
    placed = (
        P("section", WIDE, None),
        P("section", None),
        P("section", None, None),
        P("section", None),
        P("section", None),
        P("section", None),
        P("section", None),
        P("section", None, None),
        P("section", WIDE, None),
        P("section", None, WIDE),
        P("section", None, WIDE),
        P("section", WIDE, None),
    )
    return jax.shard_map(
        local, mesh=finer, in_specs=placed, out_specs=P("section", WIDE, None), check_vma=False
    )
```

```python
import functools
import math

import jax
import jax.numpy as jnp
from jax import lax
from jax.experimental import pallas as pl
from jax.experimental.pallas import tpu as pltpu
from jax.sharding import Mesh
from jax.sharding import PartitionSpec as P

HEADS = 32
HEAD_DIM = 64
STATE = 64
EXPERTS = 4
TOP = 2
CAP = 40
NZ = 8
NY = 4
WIDE = ("wide_0", "wide_1")
EPSILON = 1e-05
SHIFTS = (0, 2, 6, 4)


def along_y(value, by):
    return lax.ppermute(value, "wide_1", [(y, (y + by) % NY) for y in range(NY)])


def along_z(value, target):
    return lax.ppermute(value, "wide_0", [(z, target(z) % NZ) for z in range(NZ)])


def rms_scale(values, gain_row):
    mean_sq = jnp.mean(values * values, axis=-1, keepdims=True)
    return values * lax.rsqrt(mean_sq + EPSILON) * gain_row


def route_slots(id_rows):
    flat_ids = id_rows.reshape(-1)
    one_hot = (
        flat_ids[:, None] == lax.broadcasted_iota(jnp.int32, (flat_ids.shape[0], EXPERTS), 1)
    ).astype(jnp.int32)
    running = jnp.cumsum(one_hot, axis=0) - 1
    slot_ids = jnp.sum(one_hot * running, axis=1)
    return slot_ids


def prefix_kernel(arrived_ref, out_ref):
    def step(k, carry):
        out_ref[k] = carry.astype(jnp.bfloat16)
        block = arrived_ref[k].astype(jnp.float32)
        decay = block[32:33] + block[33:34] + block[34:35]
        return carry * decay + block[:32]

    lax.fori_loop(0, NZ * NY, step, jnp.zeros((32, 128), jnp.float32), unroll=8)


def prefix_states(arrived):
    return pl.pallas_call(
        prefix_kernel,
        out_shape=jax.ShapeDtypeStruct((NZ * NY, 32, 128), jnp.bfloat16),
        in_specs=[pl.BlockSpec(memory_space=pltpu.VMEM)],
        out_specs=pl.BlockSpec(memory_space=pltpu.VMEM),
        compiler_params=pltpu.CompilerParams(vmem_limit_bytes=4 * 2**20),
        name="prefix_states",
    )(pltpu.with_memory_space_constraint(arrived, pltpu.VMEM))


def carried_states(payload):
    arrived = lax.all_to_all(payload, WIDE, split_axis=0, concat_axis=0, tiled=True)
    back = lax.all_to_all(
        prefix_states(arrived), WIDE, split_axis=0, concat_axis=0, tiled=True
    )
    return back.reshape(16, 2, 32, 128).transpose(1, 2, 0, 3).reshape(STATE, -1)


def head_column(values, head):
    lanes = lax.broadcasted_iota(jnp.int32, values.shape, 1)
    return jnp.sum(jnp.where(lanes == head, values, 0.0), axis=1, keepdims=True)


def pair_columns(values, pair):
    shape = (values.shape[0], 2 * HEAD_DIM)
    lanes = lax.broadcasted_iota(jnp.int32, shape, 1)
    return jnp.where(
        lanes < HEAD_DIM, head_column(values, 2 * pair), head_column(values, 2 * pair + 1)
    )


def ordered(seq_len):
    rows = lax.broadcasted_iota(jnp.int32, (seq_len, seq_len), 0)
    return rows >= lax.broadcasted_iota(jnp.int32, (seq_len, seq_len), 1)


def front_kernel(
    inputs_ref, gain_ref, ssm_ref, rate_ref, payload_ref, normed_ref, maps_ref, step_ref, cum_ref
):
    values = inputs_ref[...].astype(jnp.float32)
    normed = rms_scale(values, gain_ref[...]).astype(jnp.bfloat16)
    normed_ref[...] = normed
    projected = lax.dot_general(
        normed, ssm_ref[...], (((1,), (1,)), ((), ())), preferred_element_type=jnp.float32
    )
    maps_ref[...] = projected[:, : 2 * STATE]
    raw = projected[:, 2 * STATE :]
    step_size = jnp.maximum(raw, 0.0) + jnp.log1p(jnp.exp(-jnp.abs(raw)))
    step_ref[...] = step_size
    seq_len = values.shape[0]
    cumulative = jnp.dot(
        ordered(seq_len).astype(jnp.float32),
        -step_size * rate_ref[...],
        precision=lax.Precision.HIGHEST,
        preferred_element_type=jnp.float32,
    )
    cum_ref[...] = cumulative
    total = cumulative[seq_len - 1 :]
    tail = jnp.exp(total - cumulative) * step_size
    decay = jnp.exp(total)
    b_rows = (projected[:, :STATE] / float(STATE)).astype(jnp.bfloat16)
    row = lax.broadcasted_iota(jnp.int32, (8, 2 * HEAD_DIM), 0)

    def pair_step(pair, carry):
        lanes = pl.ds(pl.multiple_of(pair * 2 * HEAD_DIM, 2 * HEAD_DIM), 2 * HEAD_DIM)
        here = normed_ref[:, lanes].astype(jnp.float32)
        weighted = (pair_columns(tail, pair) * here).astype(jnp.bfloat16)
        state = lax.dot_general(
            b_rows, weighted, (((0,), (0,)), ((), ())), preferred_element_type=jnp.float32
        )
        cols = pair_columns(decay, pair)
        high = cols.astype(jnp.bfloat16).astype(jnp.float32)
        mid = (cols - high).astype(jnp.bfloat16).astype(jnp.float32)
        low = cols - high - mid
        extra = jnp.where(
            row == 0, high, jnp.where(row == 1, mid, jnp.where(row == 2, low, 0.0))
        )
        for half in range(2):
            block = jnp.concatenate([state[half * 32 : half * 32 + 32], extra], axis=0)
            payload_ref[2 * pair + half] = block.astype(jnp.bfloat16)
        return carry

    lax.fori_loop(0, HEADS // 2, pair_step, 0, unroll=4)


def within_kernel(normed_ref, maps_ref, step_ref, cum_ref, skip_ref, out_ref, cum_t, step_t):
    cumulative = cum_ref[...]
    cum_t[...] = cumulative.T
    step_t[...] = step_ref[...].T
    seq_len = cumulative.shape[0]
    mask = ordered(seq_len)
    b_rows = (maps_ref[:, :STATE] / float(STATE)).astype(jnp.bfloat16)
    c_rows = (maps_ref[:, STATE:] / math.sqrt(STATE)).astype(jnp.bfloat16)
    meets = lax.dot_general(
        c_rows, b_rows, (((1,), (1,)), ((), ())), preferred_element_type=jnp.float32
    )

    def pair_step(pair, carry):
        lanes = pl.ds(pl.multiple_of(pair * 2 * HEAD_DIM, 2 * HEAD_DIM), 2 * HEAD_DIM)
        here = normed_ref[:, lanes]
        results = []
        for side in range(2):
            head = 2 * pair + side
            gaps = head_column(cumulative, head) - cum_t[pl.ds(head, 1), :]
            kernel = jnp.where(mask, jnp.exp(jnp.where(mask, gaps, 0.0)), 0.0)
            mixing = (meets * kernel * step_t[pl.ds(head, 1), :]).astype(jnp.bfloat16)
            results.append(jnp.dot(mixing, here, preferred_element_type=jnp.float32))
        left = lax.broadcasted_iota(jnp.int32, results[0].shape, 1) < HEAD_DIM
        skip = pair_columns(skip_ref[...], pair)
        out_ref[:, lanes] = (
            jnp.where(left, results[0], results[1]) + here.astype(jnp.float32) * skip
        )
        return carry

    lax.fori_loop(0, HEADS // 2, pair_step, 0)


def mixer_block(inputs, mixer_gain, ssm_weight, decay_rate, skip_gain, mixed_gain):
    seq_len, features = inputs.shape
    here = pl.BlockSpec(memory_space=pltpu.VMEM)
    payload, normed, maps, step_size, cumulative = pl.pallas_call(
        front_kernel,
        out_shape=[
            jax.ShapeDtypeStruct((NZ * NY, 40, 2 * HEAD_DIM), jnp.bfloat16),
            jax.ShapeDtypeStruct((seq_len, features), jnp.bfloat16),
            jax.ShapeDtypeStruct((seq_len, 2 * STATE), jnp.float32),
            jax.ShapeDtypeStruct((seq_len, HEADS), jnp.float32),
            jax.ShapeDtypeStruct((seq_len, HEADS), jnp.float32),
        ],
        in_specs=[here] * 4,
        out_specs=[here] * 5,
        name="front",
    )(inputs, mixer_gain[None], ssm_weight.T, decay_rate[None])
    carried_in = carried_states(payload)
    within = pl.pallas_call(
        within_kernel,
        out_shape=jax.ShapeDtypeStruct((seq_len, features), jnp.float32),
        in_specs=[here] * 5,
        out_specs=here,
        scratch_shapes=[
            pltpu.VMEM((HEADS, seq_len), jnp.float32),
            pltpu.VMEM((HEADS, seq_len), jnp.float32),
        ],
        cost_estimate=pl.CostEstimate(
            flops=10 * seq_len * seq_len * features,
            transcendentals=seq_len * seq_len * HEADS,
            bytes_accessed=8 * seq_len * features,
        ),
        compiler_params=pltpu.CompilerParams(vmem_limit_bytes=10 * 2**20),
        name="within",
    )(normed, maps, step_size, cumulative, skip_gain[None])
    c_rows = maps[:, STATE:] / math.sqrt(STATE)
    carried_part = jnp.dot(
        c_rows.astype(jnp.bfloat16), carried_in, preferred_element_type=jnp.float32
    ) * jnp.repeat(jnp.exp(cumulative), HEAD_DIM, axis=1)
    return inputs.astype(jnp.float32) + rms_scale(within + carried_part, mixed_gain)


def expert_kernel(sizes, tile, out_tile, *refs):
    n = len(sizes)
    pieces, (gate, up, down), outs = refs[:n], refs[n : n + 3], refs[n + 3 : 2 * n + 3]
    rows, gate_up, downs, hidden, sem_in, sem_down = refs[2 * n + 3 :]
    tiles, out_tiles = gate_up.shape[0], downs.shape[0]

    def copies(i):
        cols = pl.ds(pl.multiple_of(i * tile, tile), tile)
        return (
            pltpu.make_async_copy(
                gate.at[:, cols], gate_up.at[i, :, pl.ds(0, tile)], sem_in.at[i, 0]
            ),
            pltpu.make_async_copy(
                up.at[:, cols], gate_up.at[i, :, pl.ds(tile, tile)], sem_in.at[i, 1]
            ),
        )

    def down_copy(j):
        return pltpu.make_async_copy(
            down.at[:, pl.ds(pl.multiple_of(j * out_tile, out_tile), out_tile)],
            downs.at[j],
            sem_down.at[j],
        )

    ahead = 3
    for i in range(ahead):
        for copy in copies(i):
            copy.start()
    at = 0
    for piece, size in zip(pieces, sizes):

        def gather(i, carry, piece=piece, at=at):
            rows[pl.ds(pl.multiple_of(at + i * 16, 16), 16)] = piece[
                pl.ds(pl.multiple_of(i * 16, 16), 16)
            ]
            return carry

        lax.fori_loop(0, size // 16, gather, 0)
        at += size

    def first(i, carry):
        for copy in copies(i):
            copy.wait()

        @pl.when(i + ahead < tiles)
        def _():
            for copy in copies(i + ahead):
                copy.start()

        @pl.when(i + out_tiles >= tiles)
        def _():
            down_copy(i + out_tiles - tiles).start()

        both = jnp.dot(rows[...], gate_up[i], preferred_element_type=jnp.float32)
        gate_pre, up_pre = both[:, :tile], both[:, tile:]
        hidden[:, pl.ds(pl.multiple_of(i * tile, tile), tile)] = (
            jax.nn.silu(gate_pre) * up_pre
        ).astype(jnp.bfloat16)
        return carry

    lax.fori_loop(0, tiles, first, 0)

    def second(j, carry):
        down_copy(j).wait()
        result = jnp.dot(hidden[...], downs[j], preferred_element_type=jnp.float32)
        result = result.astype(jnp.bfloat16)
        at = 0
        for out, size in zip(outs, sizes):
            out[:, pl.ds(pl.multiple_of(j * out_tile, out_tile), out_tile)] = result[at : at + size]
            at += size
        return carry

    lax.fori_loop(0, out_tiles, second, 0)


def expert_rows(pieces, *weights):
    features, width = weights[0].shape
    tile, out_tile = 128, 512
    sizes = tuple(piece.shape[0] for piece in pieces)
    total = sum(sizes)
    here = pl.BlockSpec(memory_space=pltpu.VMEM)
    away = pl.BlockSpec(memory_space=pltpu.HBM)
    return pl.pallas_call(
        functools.partial(expert_kernel, sizes, tile, out_tile),
        out_shape=[jax.ShapeDtypeStruct((size, features), jnp.bfloat16) for size in sizes],
        in_specs=[here] * len(sizes) + [away] * 3,
        out_specs=[here] * len(sizes),
        scratch_shapes=[
            pltpu.VMEM((total, features), jnp.bfloat16),
            pltpu.VMEM((width // tile, features, 2 * tile), jnp.bfloat16),
            pltpu.VMEM((features // out_tile, width, out_tile), jnp.bfloat16),
            pltpu.VMEM((total, width), jnp.bfloat16),
            pltpu.SemaphoreType.DMA((width // tile, 2)),
            pltpu.SemaphoreType.DMA((features // out_tile,)),
        ],
        compiler_params=pltpu.CompilerParams(vmem_limit_bytes=24 * 2**20),
        cost_estimate=pl.CostEstimate(
            flops=6 * total * features * width,
            transcendentals=total * width,
            bytes_accessed=6 * features * width + 4 * total * features,
        ),
        name="expert_rows",
    )(*pieces, *(pltpu.with_memory_space_constraint(w, pltpu.HBM) for w in weights))


def join_kernel(*refs):
    blocks, out = refs[:-1], refs[-1]
    rows = blocks[0].shape[0]
    for number, block in enumerate(blocks):

        def copy(i, carry, block=block, at=number * rows):
            out[pl.ds(pl.multiple_of(at + i * 8, 8), 8)] = block[pl.ds(pl.multiple_of(i * 8, 8), 8)]
            return carry

        lax.fori_loop(0, rows // 8, copy, 0)


def joined(blocks):
    rows, features = blocks[0].shape
    here = pl.BlockSpec(memory_space=pltpu.VMEM)
    return pl.pallas_call(
        join_kernel,
        out_shape=jax.ShapeDtypeStruct((rows * len(blocks), features), blocks[0].dtype),
        in_specs=[here] * len(blocks),
        out_specs=here,
        compiler_params=pltpu.CompilerParams(vmem_limit_bytes=6 * 2**20),
        name="join",
    )(*(pltpu.with_memory_space_constraint(block, pltpu.VMEM) for block in blocks))


def merge_kernel(at, whole_ref, part_ref, out_ref):
    rows = part_ref.shape[0]
    for start in range(0, whole_ref.shape[0], rows):

        def copy(i, carry, start=start):
            here = pl.ds(pl.multiple_of(start + i * 16, 16), 16)
            value = whole_ref[here]
            if start == at:
                part = part_ref[pl.ds(pl.multiple_of(i * 16, 16), 16)].astype(jnp.float32)
                value = (value.astype(jnp.float32) + part).astype(jnp.bfloat16)
            out_ref[here] = value
            return carry

        lax.fori_loop(0, rows // 16, copy, 0)


def merged(whole, part, at):
    here = pl.BlockSpec(memory_space=pltpu.VMEM)
    return pl.pallas_call(
        functools.partial(merge_kernel, at),
        out_shape=jax.ShapeDtypeStruct(whole.shape, whole.dtype),
        in_specs=[here] * 2,
        out_specs=here,
        compiler_params=pltpu.CompilerParams(vmem_limit_bytes=6 * 2**20),
        name="merge",
    )(whole, part)


def onward(value, target):
    sections = lax.axis_size("section")
    pairs = [
        (s * NZ + z, (s + 1) % sections * NZ + target(z) % NZ)
        for s in range(sections)
        for z in range(NZ)
    ]
    return lax.ppermute(value, ("section", "wide_0"), pairs)


def finish_kernel(kept_ref, *refs):
    answers, out_ref, stacked = refs[:-2], refs[-2], refs[-1]
    for number, answer in enumerate(answers):

        def copy(i, carry, answer=answer, at=number * CAP):
            stacked[pl.ds(pl.multiple_of(at + i * 8, 8), 8)] = answer[
                pl.ds(pl.multiple_of(i * 8, 8), 8)
            ]
            return carry

        lax.fori_loop(0, CAP // 8, copy, 0, unroll=True)
    features = out_ref.shape[1]
    weights = kept_ref[:, features : features + len(SHIFTS) * CAP]
    parts = [weights[:, :CAP]]
    for i in range(1, len(SHIFTS)):
        parts += [weights[:, i * CAP : (i + 1) * CAP]] * 2
    weights = jnp.concatenate(parts, axis=1)
    high = weights.astype(jnp.bfloat16)
    low = (weights - high.astype(jnp.float32)).astype(jnp.bfloat16)
    for at in range(0, features, 512):
        rows = stacked[:, at : at + 512]
        result = kept_ref[:, at : at + 512] + jnp.dot(
            high, rows, preferred_element_type=jnp.float32
        )
        result += jnp.dot(low, rows, preferred_element_type=jnp.float32)
        out_ref[:, at : at + 512] = result.astype(jnp.bfloat16)


def finished(kept, answers):
    rows, features = kept.shape[0], answers[0].shape[1]
    here = pl.BlockSpec(memory_space=pltpu.VMEM)
    return pl.pallas_call(
        finish_kernel,
        out_shape=jax.ShapeDtypeStruct((rows, features), jnp.bfloat16),
        in_specs=[here] * (1 + len(answers)),
        out_specs=here,
        scratch_shapes=[pltpu.VMEM((len(answers) * CAP, features), jnp.bfloat16)],
        compiler_params=pltpu.CompilerParams(vmem_limit_bytes=10 * 2**20),
        name="finish",
    )(*(pltpu.with_memory_space_constraint(value, pltpu.VMEM) for value in (kept, *answers)))


def weighted_rows(weights, rows):
    high = lax.reduce_precision(weights, 8, 7)
    both = [high.astype(jnp.bfloat16), (weights - high).astype(jnp.bfloat16)]
    return sum(jnp.dot(part, rows, preferred_element_type=jnp.float32) for part in both)


def expert_layer(residual, ffn_gain, router_weight, id_rows, gate_part, up_part, down_part):
    tok_rows = residual.shape[0]
    features = residual.shape[1]
    zi = lax.axis_index("wide_0")
    slots = route_slots(id_rows).reshape(tok_rows, TOP)
    routed = rms_scale(residual, ffn_gain).astype(jnp.bfloat16)
    logits = jnp.dot(routed, router_weight, preferred_element_type=jnp.float32)
    experts = lax.broadcasted_iota(jnp.int32, (tok_rows, EXPERTS), 1)
    signs = (experts == id_rows[:, :1]).astype(jnp.float32) - (
        experts == id_rows[:, 1:]
    ).astype(jnp.float32)
    first_share = jax.nn.sigmoid(jnp.sum(logits * signs, axis=1))
    shares = jnp.stack([first_share, 1.0 - first_share], axis=1)

    shifts = [jnp.full((CAP,), shift, jnp.int32) for shift in SHIFTS]
    col_expert = (zi + jnp.concatenate(shifts)) % NZ // 2
    col_slot = lax.broadcasted_iota(jnp.int32, (len(SHIFTS), CAP), 1).reshape(-1)
    hits = [
        (id_rows[:, k][:, None] == col_expert[None, :]) & (slots[:, k][:, None] == col_slot[None, :])
        for k in range(TOP)
    ]
    placing = (hits[0] | hits[1]).astype(jnp.bfloat16)
    combine = jnp.where(hits[0], shares[:, 0:1], 0.0) + jnp.where(hits[1], shares[:, 1:2], 0.0)
    packed = lax.dot_general(
        placing, routed, (((0,), (0,)), ((), ())), preferred_element_type=jnp.float32
    ).astype(jnp.bfloat16).reshape(len(SHIFTS), CAP, features)

    blocks = [packed[0]]
    for shift, block in zip(SHIFTS[1:], packed[1:]):
        blocks.append(along_z(block, lambda z, by=shift: z + by))
    even = joined(blocks)
    odd = along_z(even, lambda z: z ^ 1)

    sums = []
    for own in (even, odd):
        half = own.shape[0] // 2
        left = along_y(own, 1)
        right = along_y(own, -1)
        far_a = along_y(left[:half], 1)
        far_b = along_y(right[half:], -1)
        o_own, o_left, o_right, o_far_a, o_far_b = expert_rows(
            (own, left, right, far_a, far_b), gate_part, up_part, down_part
        )
        mid_a = along_y(o_far_a, -1)
        mid_b = along_y(o_far_b, 1)
        to_left = merged(o_left, mid_a, 0)
        to_right = merged(o_right, mid_b, half)
        from_left = along_y(to_left, -1)
        from_right = along_y(to_right, 1)
        total = o_own.astype(jnp.float32) + from_left.astype(jnp.float32)
        sums.append((total + from_right.astype(jnp.float32)).astype(jnp.bfloat16))

    own_part = residual + weighted_rows(combine[:, :CAP], sums[0][:CAP])
    spare = jnp.zeros((tok_rows, 96), jnp.float32)
    kept = onward(jnp.concatenate([own_part, combine, spare], axis=1), lambda z: z)
    answers = []
    for i, shift in enumerate(SHIFTS):
        part = slice(i * CAP, (i + 1) * CAP)
        if i:
            answers.append(onward(sums[0][part], lambda z, by=shift: z - by))
        answers.append(onward(sums[1][part], lambda z, by=shift: (z ^ 1) - by))
    return finished(kept, answers)


def local(
    stream,
    mixer_gain,
    ssm_weight,
    decay_rate,
    skip_gain,
    mixed_gain,
    ffn_gain,
    router_weight,
    expert_ids,
    gate_weight,
    up_weight,
    down_weight,
):
    residual = mixer_block(
        stream[0], mixer_gain[0], ssm_weight[0], decay_rate[0], skip_gain[0], mixed_gain[0]
    )
    result = expert_layer(
        residual,
        ffn_gain[0],
        router_weight[0],
        expert_ids[0],
        gate_weight[0],
        up_weight[0],
        down_weight[0],
    )
    return result[None]


def solution(mesh):
    finer = Mesh(
        mesh.devices.reshape(mesh.shape["section"], NZ, NY), ("section", "wide_0", "wide_1")
    )
    placed = (
        P("section", WIDE, None),
        P("section", None),
        P("section", None, None),
        P("section", None),
        P("section", None),
        P("section", None),
        P("section", None),
        P("section", None, None),
        P("section", WIDE, None),
        P("section", None, WIDE),
        P("section", None, WIDE),
        P("section", WIDE, None),
    )
    return jax.shard_map(
        local, mesh=finer, in_specs=placed, out_specs=P("section", WIDE, None), check_vma=False
    )
```

```python
import functools
import math

import jax
import jax.numpy as jnp
from jax import lax
from jax.experimental import pallas as pl
from jax.experimental.pallas import tpu as pltpu
from jax.sharding import Mesh
from jax.sharding import PartitionSpec as P

HEADS = 32
HEAD_DIM = 64
STATE = 64
EXPERTS = 4
TOP = 2
CAP = 40
NZ = 8
NY = 4
WIDE = ("wide_0", "wide_1")
EPSILON = 1e-05
SHIFTS = (0, 2, 6, 4)


def along_y(value, by):
    return lax.ppermute(value, "wide_1", [(y, (y + by) % NY) for y in range(NY)])


def along_z(value, target):
    return lax.ppermute(value, "wide_0", [(z, target(z) % NZ) for z in range(NZ)])


def rms_scale(values, gain_row):
    mean_sq = jnp.mean(values * values, axis=-1, keepdims=True)
    return values * lax.rsqrt(mean_sq + EPSILON) * gain_row


def route_slots(id_rows):
    flat_ids = id_rows.reshape(-1)
    one_hot = (
        flat_ids[:, None] == lax.broadcasted_iota(jnp.int32, (flat_ids.shape[0], EXPERTS), 1)
    ).astype(jnp.int32)
    running = jnp.cumsum(one_hot, axis=0) - 1
    slot_ids = jnp.sum(one_hot * running, axis=1)
    return slot_ids


def prefix_kernel(arrived_ref, out_ref):
    def step(k, carry):
        out_ref[k] = carry.astype(jnp.bfloat16)
        block = arrived_ref[k].astype(jnp.float32)
        decay = block[32:33] + block[33:34] + block[34:35]
        return carry * decay + block[:32]

    lax.fori_loop(0, NZ * NY, step, jnp.zeros((32, 128), jnp.float32), unroll=8)


def prefix_states(arrived):
    return pl.pallas_call(
        prefix_kernel,
        out_shape=jax.ShapeDtypeStruct((NZ * NY, 32, 128), jnp.bfloat16),
        in_specs=[pl.BlockSpec(memory_space=pltpu.VMEM)],
        out_specs=pl.BlockSpec(memory_space=pltpu.VMEM),
        compiler_params=pltpu.CompilerParams(vmem_limit_bytes=4 * 2**20),
        name="prefix_states",
    )(pltpu.with_memory_space_constraint(arrived, pltpu.VMEM))


def carried_states(payload):
    arrived = lax.all_to_all(payload, WIDE, split_axis=0, concat_axis=0, tiled=True)
    back = lax.all_to_all(
        prefix_states(arrived), WIDE, split_axis=0, concat_axis=0, tiled=True
    )
    return back.reshape(16, 2, 32, 128).transpose(1, 2, 0, 3).reshape(STATE, -1)


def head_column(values, head):
    lanes = lax.broadcasted_iota(jnp.int32, values.shape, 1)
    return jnp.sum(jnp.where(lanes == head, values, 0.0), axis=1, keepdims=True)


def pair_columns(values, pair):
    shape = (values.shape[0], 2 * HEAD_DIM)
    lanes = lax.broadcasted_iota(jnp.int32, shape, 1)
    return jnp.where(
        lanes < HEAD_DIM, head_column(values, 2 * pair), head_column(values, 2 * pair + 1)
    )


def ordered(seq_len):
    rows = lax.broadcasted_iota(jnp.int32, (seq_len, seq_len), 0)
    return rows >= lax.broadcasted_iota(jnp.int32, (seq_len, seq_len), 1)


def front_kernel(
    inputs_ref, gain_ref, ssm_ref, rate_ref, payload_ref, normed_ref, maps_ref, step_ref, cum_ref
):
    values = inputs_ref[...].astype(jnp.float32)
    normed = rms_scale(values, gain_ref[...]).astype(jnp.bfloat16)
    normed_ref[...] = normed
    projected = lax.dot_general(
        normed, ssm_ref[...], (((1,), (1,)), ((), ())), preferred_element_type=jnp.float32
    )
    maps_ref[...] = projected[:, : 2 * STATE]
    raw = projected[:, 2 * STATE :]
    step_size = jnp.maximum(raw, 0.0) + jnp.log1p(jnp.exp(-jnp.abs(raw)))
    step_ref[...] = step_size
    seq_len = values.shape[0]
    cumulative = jnp.dot(
        ordered(seq_len).astype(jnp.float32),
        -step_size * rate_ref[...],
        precision=lax.Precision.HIGHEST,
        preferred_element_type=jnp.float32,
    )
    cum_ref[...] = cumulative
    total = cumulative[seq_len - 1 :]
    tail = jnp.exp(total - cumulative) * step_size
    decay = jnp.exp(total)
    b_rows = (projected[:, :STATE] / float(STATE)).astype(jnp.bfloat16)
    row = lax.broadcasted_iota(jnp.int32, (8, 2 * HEAD_DIM), 0)

    def pair_step(pair, carry):
        lanes = pl.ds(pl.multiple_of(pair * 2 * HEAD_DIM, 2 * HEAD_DIM), 2 * HEAD_DIM)
        here = normed_ref[:, lanes].astype(jnp.float32)
        weighted = (pair_columns(tail, pair) * here).astype(jnp.bfloat16)
        state = lax.dot_general(
            b_rows, weighted, (((0,), (0,)), ((), ())), preferred_element_type=jnp.float32
        )
        cols = pair_columns(decay, pair)
        high = cols.astype(jnp.bfloat16).astype(jnp.float32)
        mid = (cols - high).astype(jnp.bfloat16).astype(jnp.float32)
        low = cols - high - mid
        extra = jnp.where(
            row == 0, high, jnp.where(row == 1, mid, jnp.where(row == 2, low, 0.0))
        )
        for half in range(2):
            block = jnp.concatenate([state[half * 32 : half * 32 + 32], extra], axis=0)
            payload_ref[2 * pair + half] = block.astype(jnp.bfloat16)
        return carry

    lax.fori_loop(0, HEADS // 2, pair_step, 0, unroll=4)


def within_kernel(normed_ref, maps_ref, step_ref, cum_ref, skip_ref, out_ref, cum_t, step_t):
    cumulative = cum_ref[...]
    cum_t[...] = cumulative.T
    step_t[...] = step_ref[...].T
    seq_len = cumulative.shape[0]
    mask = ordered(seq_len)
    b_rows = (maps_ref[:, :STATE] / float(STATE)).astype(jnp.bfloat16)
    c_rows = (maps_ref[:, STATE:] / math.sqrt(STATE)).astype(jnp.bfloat16)
    meets = lax.dot_general(
        c_rows, b_rows, (((1,), (1,)), ((), ())), preferred_element_type=jnp.float32
    )

    def pair_step(pair, carry):
        lanes = pl.ds(pl.multiple_of(pair * 2 * HEAD_DIM, 2 * HEAD_DIM), 2 * HEAD_DIM)
        here = normed_ref[:, lanes]
        results = []
        for side in range(2):
            head = 2 * pair + side
            gaps = head_column(cumulative, head) - cum_t[pl.ds(head, 1), :]
            kernel = jnp.where(mask, jnp.exp(jnp.where(mask, gaps, 0.0)), 0.0)
            mixing = (meets * kernel * step_t[pl.ds(head, 1), :]).astype(jnp.bfloat16)
            results.append(jnp.dot(mixing, here, preferred_element_type=jnp.float32))
        left = lax.broadcasted_iota(jnp.int32, results[0].shape, 1) < HEAD_DIM
        skip = pair_columns(skip_ref[...], pair)
        out_ref[:, lanes] = (
            jnp.where(left, results[0], results[1]) + here.astype(jnp.float32) * skip
        )
        return carry

    lax.fori_loop(0, HEADS // 2, pair_step, 0)


def mixer_block(inputs, mixer_gain, ssm_weight, decay_rate, skip_gain, mixed_gain):
    seq_len, features = inputs.shape
    here = pl.BlockSpec(memory_space=pltpu.VMEM)
    payload, normed, maps, step_size, cumulative = pl.pallas_call(
        front_kernel,
        out_shape=[
            jax.ShapeDtypeStruct((NZ * NY, 40, 2 * HEAD_DIM), jnp.bfloat16),
            jax.ShapeDtypeStruct((seq_len, features), jnp.bfloat16),
            jax.ShapeDtypeStruct((seq_len, 2 * STATE), jnp.float32),
            jax.ShapeDtypeStruct((seq_len, HEADS), jnp.float32),
            jax.ShapeDtypeStruct((seq_len, HEADS), jnp.float32),
        ],
        in_specs=[here] * 4,
        out_specs=[here] * 5,
        name="front",
    )(inputs, mixer_gain[None], ssm_weight.T, decay_rate[None])
    carried_in = carried_states(payload)
    within = pl.pallas_call(
        within_kernel,
        out_shape=jax.ShapeDtypeStruct((seq_len, features), jnp.float32),
        in_specs=[here] * 5,
        out_specs=here,
        scratch_shapes=[
            pltpu.VMEM((HEADS, seq_len), jnp.float32),
            pltpu.VMEM((HEADS, seq_len), jnp.float32),
        ],
        cost_estimate=pl.CostEstimate(
            flops=10 * seq_len * seq_len * features,
            transcendentals=seq_len * seq_len * HEADS,
            bytes_accessed=8 * seq_len * features,
        ),
        compiler_params=pltpu.CompilerParams(vmem_limit_bytes=10 * 2**20),
        name="within",
    )(normed, maps, step_size, cumulative, skip_gain[None])
    c_rows = maps[:, STATE:] / math.sqrt(STATE)
    carried_part = jnp.dot(
        c_rows.astype(jnp.bfloat16), carried_in, preferred_element_type=jnp.float32
    ) * jnp.repeat(jnp.exp(cumulative), HEAD_DIM, axis=1)
    return inputs.astype(jnp.float32) + rms_scale(within + carried_part, mixed_gain)


def expert_kernel(sizes, out_sizes, tile, out_tile, *refs):
    n, scratch = len(sizes), len(refs) - 6
    pieces, (gate, up, down), outs = refs[:n], refs[n : n + 3], refs[n + 3 : scratch]
    rows, gate_up, downs, hidden, sem_in, sem_down = refs[scratch:]
    tiles, out_tiles = gate_up.shape[0], downs.shape[0]

    def copies(i):
        cols = pl.ds(pl.multiple_of(i * tile, tile), tile)
        return (
            pltpu.make_async_copy(
                gate.at[:, cols], gate_up.at[i, :, pl.ds(0, tile)], sem_in.at[i, 0]
            ),
            pltpu.make_async_copy(
                up.at[:, cols], gate_up.at[i, :, pl.ds(tile, tile)], sem_in.at[i, 1]
            ),
        )

    def down_copy(j):
        return pltpu.make_async_copy(
            down.at[:, pl.ds(pl.multiple_of(j * out_tile, out_tile), out_tile)],
            downs.at[j],
            sem_down.at[j],
        )

    ahead = 3
    for i in range(ahead):
        for copy in copies(i):
            copy.start()
    at = 0
    for piece, size in zip(pieces, sizes):

        def gather(i, carry, piece=piece, at=at):
            rows[pl.ds(pl.multiple_of(at + i * 16, 16), 16)] = piece[
                pl.ds(pl.multiple_of(i * 16, 16), 16)
            ]
            return carry

        lax.fori_loop(0, size // 16, gather, 0)
        at += size

    def first(i, carry):
        for copy in copies(i):
            copy.wait()

        @pl.when(i + ahead < tiles)
        def _():
            for copy in copies(i + ahead):
                copy.start()

        @pl.when(i + out_tiles >= tiles)
        def _():
            down_copy(i + out_tiles - tiles).start()

        both = jnp.dot(rows[...], gate_up[i], preferred_element_type=jnp.float32)
        gate_pre, up_pre = both[:, :tile], both[:, tile:]
        hidden[:, pl.ds(pl.multiple_of(i * tile, tile), tile)] = (
            jax.nn.silu(gate_pre) * up_pre
        ).astype(jnp.bfloat16)
        return carry

    lax.fori_loop(0, tiles, first, 0)

    def second(j, carry):
        down_copy(j).wait()
        result = jnp.dot(hidden[...], downs[j], preferred_element_type=jnp.float32)
        result = result.astype(jnp.bfloat16)
        at = 0
        for out, size in zip(outs, out_sizes):
            out[:, pl.ds(pl.multiple_of(j * out_tile, out_tile), out_tile)] = result[at : at + size]
            at += size
        return carry

    lax.fori_loop(0, out_tiles, second, 0)


def expert_rows(pieces, *weights):
    features, width = weights[0].shape
    tile, out_tile = 128, 512
    sizes = tuple(piece.shape[0] for piece in pieces)
    total = sum(sizes)
    out_sizes = (sizes[0] // 2,) * (2 * total // sizes[0])
    here = pl.BlockSpec(memory_space=pltpu.VMEM)
    away = pl.BlockSpec(memory_space=pltpu.HBM)
    return pl.pallas_call(
        functools.partial(expert_kernel, sizes, out_sizes, tile, out_tile),
        out_shape=[jax.ShapeDtypeStruct((size, features), jnp.bfloat16) for size in out_sizes],
        in_specs=[here] * len(sizes) + [away] * 3,
        out_specs=[here] * len(out_sizes),
        scratch_shapes=[
            pltpu.VMEM((total, features), jnp.bfloat16),
            pltpu.VMEM((width // tile, features, 2 * tile), jnp.bfloat16),
            pltpu.VMEM((features // out_tile, width, out_tile), jnp.bfloat16),
            pltpu.VMEM((total, width), jnp.bfloat16),
            pltpu.SemaphoreType.DMA((width // tile, 2)),
            pltpu.SemaphoreType.DMA((features // out_tile,)),
        ],
        compiler_params=pltpu.CompilerParams(vmem_limit_bytes=24 * 2**20),
        cost_estimate=pl.CostEstimate(
            flops=6 * total * features * width,
            transcendentals=total * width,
            bytes_accessed=6 * features * width + 4 * total * features,
        ),
        name="expert_rows",
    )(*pieces, *(pltpu.with_memory_space_constraint(w, pltpu.HBM) for w in weights))


def join_kernel(*refs):
    blocks, out = refs[:-1], refs[-1]
    rows = blocks[0].shape[0]
    for number, block in enumerate(blocks):

        def copy(i, carry, block=block, at=number * rows):
            out[pl.ds(pl.multiple_of(at + i * 8, 8), 8)] = block[pl.ds(pl.multiple_of(i * 8, 8), 8)]
            return carry

        lax.fori_loop(0, rows // 8, copy, 0)


def joined(blocks):
    rows, features = blocks[0].shape
    here = pl.BlockSpec(memory_space=pltpu.VMEM)
    return pl.pallas_call(
        join_kernel,
        out_shape=jax.ShapeDtypeStruct((rows * len(blocks), features), blocks[0].dtype),
        in_specs=[here] * len(blocks),
        out_specs=here,
        compiler_params=pltpu.CompilerParams(vmem_limit_bytes=6 * 2**20),
        name="join",
    )(*(pltpu.with_memory_space_constraint(block, pltpu.VMEM) for block in blocks))


def added(*parts):
    return sum(part.astype(jnp.float32) for part in parts).astype(jnp.bfloat16)


def onward(value, target):
    sections = lax.axis_size("section")
    pairs = [
        (s * NZ + z, (s + 1) % sections * NZ + target(z) % NZ)
        for s in range(sections)
        for z in range(NZ)
    ]
    return lax.ppermute(value, ("section", "wide_0"), pairs)


def finish_kernel(kept_ref, *refs):
    answers, out_ref, stacked = refs[:-2], refs[-2], refs[-1]
    for number, answer in enumerate(answers):

        def copy(i, carry, answer=answer, at=number * CAP):
            stacked[pl.ds(pl.multiple_of(at + i * 8, 8), 8)] = answer[
                pl.ds(pl.multiple_of(i * 8, 8), 8)
            ]
            return carry

        lax.fori_loop(0, CAP // 8, copy, 0, unroll=True)
    features = out_ref.shape[1]
    weights = kept_ref[:, features : features + len(SHIFTS) * CAP]
    parts = [weights[:, :CAP]]
    for i in range(1, len(SHIFTS)):
        parts += [weights[:, i * CAP : (i + 1) * CAP]] * 2
    weights = jnp.concatenate(parts, axis=1)
    high = weights.astype(jnp.bfloat16)
    low = (weights - high.astype(jnp.float32)).astype(jnp.bfloat16)
    for at in range(0, features, 512):
        rows = stacked[:, at : at + 512]
        result = kept_ref[:, at : at + 512] + jnp.dot(
            high, rows, preferred_element_type=jnp.float32
        )
        result += jnp.dot(low, rows, preferred_element_type=jnp.float32)
        out_ref[:, at : at + 512] = result.astype(jnp.bfloat16)


def finished(kept, answers):
    rows, features = kept.shape[0], answers[0].shape[1]
    here = pl.BlockSpec(memory_space=pltpu.VMEM)
    return pl.pallas_call(
        finish_kernel,
        out_shape=jax.ShapeDtypeStruct((rows, features), jnp.bfloat16),
        in_specs=[here] * (1 + len(answers)),
        out_specs=here,
        scratch_shapes=[pltpu.VMEM((len(answers) * CAP, features), jnp.bfloat16)],
        compiler_params=pltpu.CompilerParams(vmem_limit_bytes=10 * 2**20),
        name="finish",
    )(*(pltpu.with_memory_space_constraint(value, pltpu.VMEM) for value in (kept, *answers)))


def weighted_rows(weights, rows):
    high = lax.reduce_precision(weights, 8, 7)
    both = [high.astype(jnp.bfloat16), (weights - high).astype(jnp.bfloat16)]
    return sum(jnp.dot(part, rows, preferred_element_type=jnp.float32) for part in both)


def expert_layer(residual, ffn_gain, router_weight, id_rows, gate_part, up_part, down_part):
    tok_rows = residual.shape[0]
    features = residual.shape[1]
    zi = lax.axis_index("wide_0")
    slots = route_slots(id_rows).reshape(tok_rows, TOP)
    routed = rms_scale(residual, ffn_gain).astype(jnp.bfloat16)
    logits = jnp.dot(routed, router_weight, preferred_element_type=jnp.float32)
    experts = lax.broadcasted_iota(jnp.int32, (tok_rows, EXPERTS), 1)
    signs = (experts == id_rows[:, :1]).astype(jnp.float32) - (
        experts == id_rows[:, 1:]
    ).astype(jnp.float32)
    first_share = jax.nn.sigmoid(jnp.sum(logits * signs, axis=1))
    shares = jnp.stack([first_share, 1.0 - first_share], axis=1)

    shifts = [jnp.full((CAP,), shift, jnp.int32) for shift in SHIFTS]
    col_expert = (zi + jnp.concatenate(shifts)) % NZ // 2
    col_slot = lax.broadcasted_iota(jnp.int32, (len(SHIFTS), CAP), 1).reshape(-1)
    hits = [
        (id_rows[:, k][:, None] == col_expert[None, :]) & (slots[:, k][:, None] == col_slot[None, :])
        for k in range(TOP)
    ]
    placing = (hits[0] | hits[1]).astype(jnp.bfloat16)
    combine = jnp.where(hits[0], shares[:, 0:1], 0.0) + jnp.where(hits[1], shares[:, 1:2], 0.0)
    packed = lax.dot_general(
        placing, routed, (((0,), (0,)), ((), ())), preferred_element_type=jnp.float32
    ).astype(jnp.bfloat16).reshape(len(SHIFTS), CAP, features)

    blocks = [packed[0]]
    for shift, block in zip(SHIFTS[1:], packed[1:]):
        blocks.append(along_z(block, lambda z, by=shift: z + by))
    even = joined(blocks)
    odd = along_z(even, lambda z: z ^ 1)

    sums, fars = [], None
    for own in (even, odd):
        half = own.shape[0] // 2
        left = along_y(own, 1)
        right = along_y(own, -1)
        if fars is None:
            far_a = along_y(left[:half], 1)
            far_b = along_y(right[half:], -1)
            fars = (far_a, far_b)
        else:
            far_a = along_z(fars[0], lambda z: z ^ 1)
            far_b = along_z(fars[1], lambda z: z ^ 1)
        own_a, own_b, left_a, left_b, right_a, right_b, far_a, far_b = expert_rows(
            (own, left, right, far_a, far_b), gate_part, up_part, down_part
        )
        mid_a = along_y(far_a, -1)
        mid_b = along_y(far_b, 1)
        early_left = along_y(left_b, -1)
        early_right = along_y(right_a, 1)
        left_a = added(left_a, mid_a)
        right_b = added(right_b, mid_b)
        back_left = along_y(left_a, -1)
        back_right = along_y(right_b, 1)
        sums.append((added(own_a, back_left, early_right), added(own_b, early_left, back_right)))

    own_part = residual + weighted_rows(combine[:, :CAP], sums[0][0][:CAP])
    spare = jnp.zeros((tok_rows, 96), jnp.float32)
    kept = onward(jnp.concatenate([own_part, combine, spare], axis=1), lambda z: z)
    answers = []
    for i, shift in enumerate(SHIFTS):
        part = slice(i % 2 * CAP, (i % 2 + 1) * CAP)
        even, odd = sums[0][i // 2][part], sums[1][i // 2][part]
        if i:
            answers.append(onward(even, lambda z, by=shift: z - by))
        answers.append(onward(odd, lambda z, by=shift: (z ^ 1) - by))
    return finished(kept, answers)


def local(
    stream,
    mixer_gain,
    ssm_weight,
    decay_rate,
    skip_gain,
    mixed_gain,
    ffn_gain,
    router_weight,
    expert_ids,
    gate_weight,
    up_weight,
    down_weight,
):
    residual = mixer_block(
        stream[0], mixer_gain[0], ssm_weight[0], decay_rate[0], skip_gain[0], mixed_gain[0]
    )
    result = expert_layer(
        residual,
        ffn_gain[0],
        router_weight[0],
        expert_ids[0],
        gate_weight[0],
        up_weight[0],
        down_weight[0],
    )
    return result[None]


def solution(mesh):
    finer = Mesh(
        mesh.devices.reshape(mesh.shape["section"], NZ, NY), ("section", "wide_0", "wide_1")
    )
    placed = (
        P("section", WIDE, None),
        P("section", None),
        P("section", None, None),
        P("section", None),
        P("section", None),
        P("section", None),
        P("section", None),
        P("section", None, None),
        P("section", WIDE, None),
        P("section", None, WIDE),
        P("section", None, WIDE),
        P("section", WIDE, None),
    )
    return jax.shard_map(
        local, mesh=finer, in_specs=placed, out_specs=P("section", WIDE, None), check_vma=False
    )
```
